32 devices in a mesh: dp: 2 (over x), tp: 4 (over z), ep: 4 (over y, core).
Axes of the slice: x: 2, y: 2, z: 4, core: 2. Of those that a mesh axis runs over, the one named last changes fastest.
Arguments:
- tokens: bfloat16 [16384, 1024], P(('dp', 'ep', 'tp')), parts along dimension 0
- expert_ids: int32 [16384, 8], P(('dp', 'ep', 'tp')), parts along dimension 0
- gates: float32 [16384, 8], P(('dp', 'ep', 'tp')), parts along dimension 0
- w_gate: bfloat16 [32, 1024, 512], P('ep', None, 'tp')
- w_up: bfloat16 [32, 1024, 512], P('ep', None, 'tp')
- w_down: bfloat16 [32, 512, 1024], P('ep', 'tp')
Outputs:
- output: bfloat16 [16384, 1024], P(('dp', 'ep', 'tp')), parts along dimension 0
There are 2 independent parts. The reference program is written for one: setup_inputs(seed, part) draws one part's arguments, and reference() takes and returns one part's arrays. A program takes and returns all parts, laid end to end along the dimension named above; an argument that names none is the same for every part.
All inputs are finite; a program needn't handle non-finite values.
Results may differ from the reference program's by a relative error of at most 0.001.
Values are sent between devices in bfloat16 or wider.
A program may use at most 1 GiB of HBM per device.

```python
import jax
import jax.numpy as jnp
from jax import lax

TOKENS_DEV = 512
HIDDEN = 1024
EXPERT_FF = 512
EXPERTS = 32
TOP_K = 8
EP_SIZE = 4
TP_SIZE = 4

TOKENS = TOKENS_DEV * EP_SIZE * TP_SIZE
SPREAD = min(TOP_K, EP_SIZE)


def routing_ids(base_key):
    group_devices = EP_SIZE * TP_SIZE
    class_rows = TOKENS_DEV // EP_SIZE
    local_count = EXPERTS // EP_SIZE
    key_rows, key_target, key_rot = jax.random.split(base_key, 3)
    row_order = jax.vmap(lambda sub_key: jax.random.permutation(sub_key, TOKENS_DEV))(jax.random.split(key_rows, group_devices))
    ep_order = jax.vmap(lambda sub_key: jax.random.permutation(sub_key, EP_SIZE))(jax.random.split(key_target, group_devices))
    rotation = jax.random.randint(key_rot, (), 0, local_count)
    slots = jnp.arange(TOP_K)
    ep_class = row_order % EP_SIZE
    within = row_order // EP_SIZE + jnp.arange(group_devices)[:, None] * class_rows
    place = (ep_class[:, :, None] + slots % SPREAD) % EP_SIZE
    target_ep = jax.vmap(lambda order_row, place_rows: order_row[place_rows])(ep_order, place)
    local_slot = (within[:, :, None] + slots // SPREAD + rotation) % local_count
    return (target_ep * local_count + local_slot).astype(jnp.int32).reshape(TOKENS, TOP_K)


def setup_inputs(seed: int = 0, part: int = 0) -> dict:
    base_key = jax.random.key(seed)
    key_gate_w, key_up_w, key_down_w, key_part = jax.random.split(base_key, 4)
    key_tokens, key_ids, key_gates = jax.random.split(jax.random.fold_in(key_part, part), 3)
    tokens = jax.random.normal(key_tokens, (TOKENS, HIDDEN), jnp.float32).astype(jnp.bfloat16)
    expert_ids = routing_ids(key_ids)
    gates = jax.random.uniform(key_gates, (TOKENS, TOP_K), jnp.float32, 0.5, 1.5)
    w_gate = (jax.random.normal(key_gate_w, (EXPERTS, HIDDEN, EXPERT_FF), jnp.float32) * HIDDEN ** -0.5).astype(jnp.bfloat16)
    w_up = (jax.random.normal(key_up_w, (EXPERTS, HIDDEN, EXPERT_FF), jnp.float32) * HIDDEN ** -0.5).astype(jnp.bfloat16)
    w_down = (jax.random.normal(key_down_w, (EXPERTS, EXPERT_FF, HIDDEN), jnp.float32) * EXPERT_FF ** -0.5).astype(jnp.bfloat16)
    return {"tokens": tokens, "expert_ids": expert_ids, "gates": gates, "w_gate": w_gate, "w_up": w_up, "w_down": w_down}


def reference(tokens, expert_ids, gates, w_gate, w_up, w_down):
    load = TOKENS * TOP_K // EXPERTS
    order = jnp.argsort(expert_ids.reshape(-1), stable=True).reshape(EXPERTS, load)
    row_index = order // TOP_K
    gate_sorted = gates.reshape(-1)[order]

    def expert_out(operands):
        rows_in, gate_in, gate_mat, up_mat, down_mat = operands
        x_rows = tokens[rows_in]
        hidden_gate = jnp.dot(x_rows, gate_mat, preferred_element_type=jnp.float32)
        hidden_up = jnp.dot(x_rows, up_mat, preferred_element_type=jnp.float32)
        act_rows = (jax.nn.silu(hidden_gate) * hidden_up).astype(jnp.bfloat16)
        out_rows = jnp.dot(act_rows, down_mat, preferred_element_type=jnp.float32)
        return out_rows * gate_in[:, None]

    weighted = lax.map(expert_out, (row_index, gate_sorted, w_gate, w_up, w_down))
    summed = jax.ops.segment_sum(weighted.reshape(-1, HIDDEN), row_index.reshape(-1), num_segments=TOKENS)
    return summed.astype(jnp.bfloat16)
```

```python
import functools

import jax
import jax.numpy as jnp
from jax import lax
from jax.experimental import pallas as pl
from jax.experimental.pallas import tpu as pltpu
from jax.sharding import PartitionSpec as P

MESH = pl.DeviceIdType.MESH
F32 = jnp.float32
BF16 = jnp.bfloat16

Z_STEPS = (15, 16, 16, 17, 20, 24, 28, 32, 36, 40, 44, 48)
X_STEPS = (18, 28, 41, 53)
CHUNKS = 8


def layer_kernel(
    tok_h, gt_h, wg_h, wu_h, wd_h, out_ref,
    tok, gtb, gm, wg, wu, wd, acc, got_a, got_b, got_c,
    loc_sem, tok_ss, tok_rs, own_ss, own_rs, z_ss, q_rs, x_ss, c_ss, c_rs, out_ss, out_rs,
):
    n_own = wg_h.shape[0]
    half = n_own // 2
    rows = tok_h.shape[0]
    hidden = tok_h.shape[1]
    chunk = rows // CHUNKS
    x = lax.axis_index("dp")
    z = lax.axis_index("tp")
    ep = lax.axis_index("ep")
    core = lax.rem(ep, 2)
    to_x = {"dp": 1 - x}
    to_y = {"ep": lax.rem(ep + 2, 4)}
    to_c = {"ep": ep + 1 - 2 * core}
    to_z = {"tp": z + 1 - 2 * lax.rem(z, 2)}
    to_zz = {"tp": lax.rem(z + 2, 4)}

    def rcopy(src, dst, ss, rs, dev):
        return pltpu.make_async_remote_copy(
            src_ref=src, dst_ref=dst, send_sem=ss, recv_sem=rs, device_id=dev, device_id_type=MESH
        )

    bufs = (wg, wu, wd)
    hbm = (wg_h, wu_h, wd_h)

    loc = [
        pltpu.make_async_copy(tok_h, tok.at[0], loc_sem.at[0]),
        pltpu.make_async_copy(gt_h, gtb.at[0], loc_sem.at[1]),
    ] + [pltpu.make_async_copy(hbm[a], bufs[a].at[0, 0], loc_sem.at[2 + a]) for a in range(3)]
    for cp in loc:
        cp.start()

    barrier = pltpu.get_barrier_semaphore()
    for dev in (to_x, to_y, to_c, to_z, to_zz):
        pl.semaphore_signal(barrier, inc=1, device_id=dev, device_id_type=MESH)
    pl.semaphore_wait(barrier, 5)

    tok_y = [rcopy(tok_h, tok.at[1], tok_ss.at[0], tok_rs.at[0], to_y),
             rcopy(gt_h, gtb.at[1], tok_ss.at[1], tok_rs.at[1], to_y)]
    tok_z = [rcopy(tok_h, tok.at[2], tok_ss.at[2], tok_rs.at[2], to_zz),
             rcopy(gt_h, gtb.at[2], tok_ss.at[3], tok_rs.at[3], to_zz)]
    tok_f = [rcopy(tok.at[2], tok.at[3], tok_ss.at[4], tok_rs.at[4], to_y),
             rcopy(gtb.at[2], gtb.at[3], tok_ss.at[5], tok_rs.at[5], to_y)]

    def own_c(i, a):
        return rcopy(hbm[a].at[i], bufs[a].at[0, 1, i], own_ss.at[i, a], own_rs.at[i, a], to_c)

    def over_z(i, a):
        return rcopy(hbm[a].at[x * half + i], bufs[a].at[1, 0, 2 * i], z_ss.at[i, a], q_rs.at[2 * i, a], to_z)

    def over_x(i, a):
        return rcopy(bufs[a].at[1, 0, 2 * i], bufs[a].at[1, 0, 2 * i + 1], x_ss.at[i, a], q_rs.at[2 * i + 1, a], to_x)

    def over_c(q, a):
        return rcopy(bufs[a].at[1, 0, q], bufs[a].at[1, 1, q], c_ss.at[q, a], c_rs.at[q, a], to_c)

    for cp in tok_y + tok_z:
        cp.start()
    for a in range(3):
        own_c(0, a).start()
    for i in range(half):
        for a in range(3):
            over_z(i, a).start()
    for i in range(1, n_own):
        for a in range(3):
            own_c(i, a).start()

    def zero(t, carry):
        acc[pl.ds(t, 1)] = jnp.zeros((1,) + acc.shape[1:], F32)
        return carry

    lax.fori_loop(0, acc.shape[0], zero, 0)

    def gates_of(b):
        part = gtb[b]
        full = jnp.concatenate([part, jnp.zeros((128 - part.shape[0], rows), F32)], axis=0)
        gm[b] = full.T

    for cp in loc:
        cp.wait()
    gates_of(0)

    base = (ep * n_own, (ep + 1 - 2 * core) * n_own)
    lane = lax.broadcasted_iota(jnp.int32, (rows, 128), 1)
    cols = min(256, hidden)

    def step(k, carry):
        s = k // 32
        b = (1 - s) * (k // 8) + s * (3 - k % 4)
        i = (1 - s) * (k % 8) + s * ((k - 32) // 4)
        expert = (1 - s) * i + s * (((x + i) % 2) * half + i // 2)

        @pl.when(k < n_own)
        def _():
            for a in range(3):
                own_c(i, a).wait_recv()

        @pl.when(k == 8)
        def _():
            for cp in tok_y:
                cp.wait_recv()
            gates_of(1)

        for n, at in enumerate(Z_STEPS):
            @pl.when(k == at)
            def _(n=n):
                u, a = n // 3, n % 3
                over_z(u, a).wait_recv()
                over_x(u, a).start()
                over_c(2 * u, a).start()

        @pl.when(k == 16)
        def _():
            for cp in tok_z:
                cp.wait_recv()
            for cp in tok_f:
                cp.start()
            gates_of(2)

        @pl.when(k == 24)
        def _():
            for cp in tok_f:
                cp.wait_recv()
            gates_of(3)

        for u, at in enumerate(X_STEPS):
            @pl.when(k == at)
            def _(u=u):
                for a in range(3):
                    over_x(u, a).wait_recv()
                    over_c(2 * u + 1, a).start()

        @pl.when((k >= 32) & (k % 4 == 0))
        def _():
            for a in range(3):
                over_c((k - 32) // 4, a).wait_recv()

        xb = tok[b]
        gates = gm[b]
        hs, gs = [], []
        for c in range(2):
            w_in = jnp.concatenate([wg[s, c, i], wu[s, c, i]], axis=1)
            both = jnp.dot(xb, w_in, preferred_element_type=F32)
            f = both.shape[1] // 2
            hs.append((jax.nn.silu(both[:, :f]) * both[:, f:]).astype(BF16))
            gs.append(jnp.sum(jnp.where(lane == base[c] + expert, gates, 0.0), axis=1, keepdims=True))
        for t in range(hidden // cols):
            sl = pl.ds(t * cols, cols)
            total = acc[b, :, sl]
            for c in range(2):
                total += gs[c] * jnp.dot(hs[c], wd[s, c, i, :, sl], preferred_element_type=F32)
            acc[b, :, sl] = total

        @pl.when(k == 60)
        def _():
            for j in range(CHUNKS):
                send_a(j).start()

        @pl.when(k == 62)
        def _():
            for j in range(CHUNKS):
                send_c(j).start()

        return carry

    def part(j):
        return pl.ds(j * chunk, chunk)

    def send_a(j):
        return rcopy(acc.at[3, part(j)], got_a.at[part(j)], out_ss.at[0, j], out_rs.at[0, j], to_y)

    def send_b(j):
        return rcopy(acc.at[2, part(j)], got_b.at[part(j)], out_ss.at[1, j], out_rs.at[1, j], to_zz)

    def send_c(j):
        return rcopy(acc.at[1, part(j)], got_c.at[part(j)], out_ss.at[2, j], out_rs.at[2, j], to_y)

    lax.fori_loop(0, 64, step, 0)

    for j in range(CHUNKS):
        send_a(j).wait_recv()
        acc[2, part(j)] = acc[2, part(j)] + got_a[part(j)]
        send_b(j).start()
    for j in range(CHUNKS):
        send_c(j).wait_recv()
        acc[0, part(j)] = acc[0, part(j)] + got_c[part(j)]
    for j in range(CHUNKS):
        send_b(j).wait_recv()
        out_ref[part(j)] = (acc[0, part(j)] + got_b[part(j)]).astype(out_ref.dtype)

    for cp in tok_y + tok_z + tok_f:
        cp.wait_send()
    for a in range(3):
        for i in range(n_own):
            own_c(i, a).wait_send()
            over_c(i, a).wait_send()
        for i in range(half):
            over_z(i, a).wait_send()
            over_x(i, a).wait_send()
    for j in range(CHUNKS):
        send_a(j).wait_send()
        send_b(j).wait_send()
        send_c(j).wait_send()


def solution(mesh):
    row_spec = P(("dp", "ep", "tp"), None)

    def local_layer(tokens, expert_ids, gates, w_gate, w_up, w_down):
        n_own = w_gate.shape[0]
        rows, hidden = tokens.shape
        ff = w_gate.shape[2]
        experts = n_own * mesh.shape["ep"]
        names = lax.broadcasted_iota(jnp.int32, (experts, 1, rows), 0)
        chosen = expert_ids.T[None] == names
        gate_of = jnp.sum(jnp.where(chosen, gates.T[None], 0.0), axis=1)
        any_spec = pl.BlockSpec(memory_space=pl.ANY)
        dma = pltpu.SemaphoreType.DMA
        return pl.pallas_call(
            layer_kernel,
            out_shape=jax.ShapeDtypeStruct((rows, hidden), jnp.bfloat16),
            in_specs=[any_spec] * 5,
            out_specs=pl.BlockSpec(memory_space=pltpu.VMEM),
            scratch_shapes=[
                pltpu.VMEM((4, rows, hidden), BF16),
                pltpu.VMEM((4, experts, rows), F32),
                pltpu.VMEM((4, rows, 128), F32),
                pltpu.VMEM((2, 2, n_own, hidden, ff), BF16),
                pltpu.VMEM((2, 2, n_own, hidden, ff), BF16),
                pltpu.VMEM((2, 2, n_own, ff, hidden), BF16),
                pltpu.VMEM((4, rows, hidden), F32),
                pltpu.VMEM((rows, hidden), F32),
                pltpu.VMEM((rows, hidden), F32),
                pltpu.VMEM((rows, hidden), F32),
                dma((5,)), dma((6,)), dma((6,)),
                dma((n_own, 3)), dma((n_own, 3)),
                dma((n_own // 2, 3)), dma((n_own, 3)), dma((n_own // 2, 3)),
                dma((n_own, 3)), dma((n_own, 3)),
                dma((3, CHUNKS)), dma((3, CHUNKS)),
            ],
            compiler_params=pltpu.CompilerParams(
                collective_id=0, has_side_effects=True, vmem_limit_bytes=66_060_288
            ),
        )(tokens, gate_of, w_gate, w_up, w_down)

    return jax.shard_map(local_layer, mesh=mesh, in_specs=(row_spec, row_spec, row_spec, P("ep", None, "tp"), P("ep", None, "tp"), P("ep", "tp", None)), out_specs=row_spec, check_vma=False)
```

```python
import functools

import jax
import jax.numpy as jnp
from jax import lax
from jax.experimental import pallas as pl
from jax.experimental.pallas import tpu as pltpu
from jax.sharding import PartitionSpec as P

MESH = pl.DeviceIdType.MESH
F32 = jnp.float32
BF16 = jnp.bfloat16

CHUNKS = 8


def layer_kernel(
    tok_h, gt_h, wg_h, wu_h, wd_h, out_ref,
    tok, gtb, gm, wg, wu, wd, hid, acc, got_a, got_b, got_c,
    loc_sem, tok_ss, tok_rs, own_ss, own_rs, z_ss, q_rs, x_ss, c_ss, c_rs, out_ss, out_rs,
):
    n_own, hidden, ff = wg_h.shape
    half = n_own // 2
    rows = tok_h.shape[0]
    part_rows = rows // 2
    chunks = CHUNKS
    chunk = rows // chunks
    x = lax.axis_index("dp")
    z = lax.axis_index("tp")
    ep = lax.axis_index("ep")
    core = lax.rem(ep, 2)
    to_x = {"dp": 1 - x}
    to_y = {"ep": lax.rem(ep + 2, 4)}
    to_c = {"ep": ep + 1 - 2 * core}
    to_z = {"tp": z + 1 - 2 * lax.rem(z, 2)}
    to_zz = {"tp": lax.rem(z + 2, 4)}
    row_d, row_c, row_b, row_a = 0, rows, 2 * rows, 3 * rows

    def rcopy(src, dst, ss, rs, dev):
        return pltpu.make_async_remote_copy(
            src_ref=src, dst_ref=dst, send_sem=ss, recv_sem=rs, device_id=dev, device_id_type=MESH
        )

    bufs = (wg, wu, wd)
    hbm = (wg_h, wu_h, wd_h)

    loc = [
        pltpu.make_async_copy(tok_h, tok.at[pl.ds(row_d, rows)], loc_sem.at[0]),
        pltpu.make_async_copy(gt_h, gtb.at[0], loc_sem.at[1]),
    ] + [pltpu.make_async_copy(hbm[a], bufs[a].at[0, 0], loc_sem.at[2 + a]) for a in range(3)]
    for cp in loc:
        cp.start()

    barrier = pltpu.get_barrier_semaphore()
    for dev in (to_x, to_y, to_c, to_z, to_zz):
        pl.semaphore_signal(barrier, inc=1, device_id=dev, device_id_type=MESH)
    with jax.named_scope("entry"):
        pl.semaphore_wait(barrier, 5)

    def part(base, p):
        return pl.ds(base + p * part_rows, part_rows)

    tok_y = [rcopy(tok_h, tok.at[pl.ds(row_c, rows)], tok_ss.at[0], tok_rs.at[0], to_y)]
    gat_y = rcopy(gt_h, gtb.at[1], tok_ss.at[1], tok_rs.at[1], to_y)
    gat_z = rcopy(gt_h, gtb.at[2], tok_ss.at[2], tok_rs.at[2], to_zz)
    gat_f = rcopy(gtb.at[2], gtb.at[3], tok_ss.at[3], tok_rs.at[3], to_y)
    tok_z = [rcopy(tok_h.at[part(0, p)], tok.at[part(row_b, p)], tok_ss.at[4 + p], tok_rs.at[4 + p], to_zz)
             for p in range(2)]
    tok_f = [rcopy(tok.at[part(row_b, p)], tok.at[part(row_a, p)], tok_ss.at[6 + p], tok_rs.at[6 + p], to_y)
             for p in range(2)]

    def own_c(i, a):
        return rcopy(hbm[a].at[i], bufs[a].at[0, 1, i], own_ss.at[i, a], own_rs.at[i, a], to_c)

    def over_z(i, a):
        return rcopy(hbm[a].at[x * half + i], bufs[a].at[1, 0, 2 * i], z_ss.at[i, a], q_rs.at[2 * i, a], to_z)

    def over_x(i, a):
        return rcopy(bufs[a].at[1, 0, 2 * i], bufs[a].at[1, 0, 2 * i + 1], x_ss.at[i, a], q_rs.at[2 * i + 1, a], to_x)

    def over_c(q, a):
        return rcopy(bufs[a].at[1, 0, q], bufs[a].at[1, 1, q], c_ss.at[q, a], c_rs.at[q, a], to_c)

    tok_z[0].start()
    gat_z.start()
    tok_y[0].start()
    gat_y.start()
    for a in range(3):
        own_c(0, a).start()
    for i in range(half):
        for a in range(3):
            over_z(i, a).start()
    for i in range(1, n_own):
        for a in range(3):
            own_c(i, a).start()
    tok_z[1].start()

    def zero(t, carry):
        acc[pl.ds(pl.multiple_of(t * rows, rows), rows)] = jnp.zeros((rows, hidden), F32)
        return carry

    lax.fori_loop(0, 4, zero, 0)

    def gates_of(b):
        block = gtb[b]
        full = jnp.concatenate([block, jnp.zeros((128 - block.shape[0], rows), F32)], axis=0)
        gm[pl.ds(b * rows, rows)] = full.T

    with jax.named_scope("loc"):
        for cp in loc:
            cp.wait()
    gates_of(0)

    base = (ep * n_own, (ep + 1 - 2 * core) * n_own)
    cols = min(256, hidden)

    def inner(xb, s, c, i):
        w_in = jnp.concatenate([wg[s, c, i], wu[s, c, i]], axis=1)
        both = jnp.dot(xb, w_in, preferred_element_type=F32)
        return (jax.nn.silu(both[:, :ff]) * both[:, ff:]).astype(BF16)

    def first(r, m, i):
        at = pl.ds(r, m)
        xb = tok[at]
        for c in range(2):
            hid[c, i, at] = inner(xb, 0, c, i)

    def second(r, m, q):
        at = pl.ds(r, m)
        i = ((x + q) % 2) * half + q // 2
        xb = tok[at]
        gates = gm[at]
        lane = lax.broadcasted_iota(jnp.int32, (m, 128), 1)
        hs, gs = [], []
        for c in range(2):
            hs.append(jnp.concatenate([hid[c, i, at], inner(xb, 1, c, q)], axis=1))
            gs.append(jnp.sum(jnp.where(lane == base[c] + i, gates, 0.0), axis=1, keepdims=True))
        for t in range(hidden // cols):
            sl = pl.ds(t * cols, cols)
            total = acc[at, sl]
            for c in range(2):
                w_out = jnp.concatenate([wd[0, c, i, :, sl], wd[1, c, q, :, sl]], axis=0)
                total += gs[c] * jnp.dot(hs[c], w_out, preferred_element_type=F32)
            acc[at, sl] = total

    def first_all(r, m):
        def go(i, carry):
            first(r, m, i)
            return carry

        lax.fori_loop(0, n_own, go, 0)

    def second_all(r, m):
        def go(q, carry):
            second(r, m, q)
            return carry

        lax.fori_loop(0, n_own, go, 0)

    def pass_z(n):
        u, a = n // 3, n % 3
        with jax.named_scope(f"ev_z{n}"):
            over_z(u, a).wait_recv()
        over_x(u, a).start()
        over_c(2 * u, a).start()

    def pass_x(u):
        with jax.named_scope(f"ev_x{u}"):
            for a in range(3):
                over_x(u, a).wait_recv()
                over_c(2 * u + 1, a).start()

    def rows_of(j):
        return pl.ds(j * chunk, chunk)

    def send_a(j):
        return rcopy(acc.at[pl.ds(row_a + j * chunk, chunk)], got_a.at[rows_of(j)], out_ss.at[0, j], out_rs.at[0, j], to_y)

    def send_b(j):
        return rcopy(acc.at[pl.ds(row_b + j * chunk, chunk)], got_b.at[rows_of(j)], out_ss.at[1, j], out_rs.at[1, j], to_zz)

    def send_c(j):
        return rcopy(acc.at[pl.ds(row_c + j * chunk, chunk)], got_c.at[rows_of(j)], out_ss.at[2, j], out_rs.at[2, j], to_y)

    def add_a(j):
        with jax.named_scope(f"late_a{j}"):
            send_a(j).wait_recv()
        at = pl.ds(row_b + j * chunk, chunk)
        acc[at] = acc[at] + got_a[rows_of(j)]
        send_b(j).start()

    def mine(i, carry):
        with jax.named_scope("ev_own"):
            for a in range(3):
                own_c(i, a).wait_recv()
        first(row_d, rows, i)
        return carry

    lax.fori_loop(0, n_own, mine, 0)

    pass_z(0)
    with jax.named_scope("ev_tok_b1"):
        tok_z[0].wait_recv()
        gat_z.wait_recv()
    tok_f[0].start()
    gat_f.start()
    gates_of(2)
    pass_z(1)
    with jax.named_scope("ev_tok_c"):
        tok_y[0].wait_recv()
        gat_y.wait_recv()
    gates_of(1)
    first_all(row_c, rows)
    pass_z(2)
    first_all(row_b, part_rows)
    pass_z(3)
    with jax.named_scope("ev_tok_a1"):
        tok_f[0].wait_recv()
        gat_f.wait_recv()
    gates_of(3)
    first_all(row_a, part_rows)
    pass_x(0)
    pass_z(4)

    def step(q, carry):
        for at, ns, us in ((1, (5,), ()), (2, (6,), ()), (3, (7,), (1,)), (4, (8,), ()), (5, (9,), (2,)),
                           (6, (10, 11), ()), (7, (), (3,))):
            @pl.when(q == at)
            def _(ns=ns, us=us):
                for n in ns:
                    pass_z(n)
                for u in us:
                    pass_x(u)

        with jax.named_scope("ev_q"):
            for a in range(3):
                over_c(q, a).wait_recv()
        second(row_a, part_rows, q)

        @pl.when(q == n_own - 1)
        def _():
            with jax.named_scope("out_a1"):
                for j in range(chunks // 4):
                    send_a(j).start()

        second(row_b, part_rows, q)
        second(row_c, rows, q)
        second(row_d, rows, q)
        return carry

    lax.fori_loop(0, n_own, step, 0)

    with jax.named_scope("ev_tok_b2"):
        tok_z[1].wait_recv()
    tok_f[1].start()
    for j in range(chunks // 4, chunks // 2):
        send_a(j).start()
    first_all(row_b + part_rows, part_rows)
    for j in range(chunks // 4):
        add_a(j)
    second_all(row_b + part_rows, part_rows)
    with jax.named_scope("ev_tok_a2"):
        tok_f[1].wait_recv()
    first_all(row_a + part_rows, part_rows)
    for j in range(chunks // 4, 3 * chunks // 8):
        add_a(j)
    second_all(row_a + part_rows, part_rows)
    with jax.named_scope("out_a2"):
        for j in range(chunks // 2, chunks):
            send_a(j).start()
    for j in range(chunks):
        send_c(j).start()
    for j in range(3 * chunks // 8, chunks):
        add_a(j)
    for j in range(chunks):
        with jax.named_scope(f"late_b{j}"):
            send_b(j).wait_recv()
        with jax.named_scope(f"late_c{j}"):
            send_c(j).wait_recv()
        out_ref[rows_of(j)] = (acc[rows_of(j)] + got_c[rows_of(j)] + got_b[rows_of(j)]).astype(out_ref.dtype)

    for cp in tok_y + tok_z + tok_f + [gat_y, gat_z, gat_f]:
        cp.wait_send()
    for a in range(3):
        for i in range(n_own):
            own_c(i, a).wait_send()
            over_c(i, a).wait_send()
        for i in range(half):
            over_z(i, a).wait_send()
            over_x(i, a).wait_send()
    for j in range(chunks):
        send_a(j).wait_send()
        send_b(j).wait_send()
        send_c(j).wait_send()


def solution(mesh):
    row_spec = P(("dp", "ep", "tp"), None)

    def local_layer(tokens, expert_ids, gates, w_gate, w_up, w_down):
        n_own = w_gate.shape[0]
        rows, hidden = tokens.shape
        ff = w_gate.shape[2]
        experts = n_own * mesh.shape["ep"]
        names = lax.broadcasted_iota(jnp.int32, (experts, 1, rows), 0)
        chosen = expert_ids.T[None] == names
        gate_of = jnp.sum(jnp.where(chosen, gates.T[None], 0.0), axis=1)
        any_spec = pl.BlockSpec(memory_space=pl.ANY)
        dma = pltpu.SemaphoreType.DMA
        return pl.pallas_call(
            layer_kernel,
            out_shape=jax.ShapeDtypeStruct((rows, hidden), jnp.bfloat16),
            in_specs=[any_spec] * 5,
            out_specs=pl.BlockSpec(memory_space=pltpu.VMEM),
            scratch_shapes=[
                pltpu.VMEM((4 * rows, hidden), BF16),
                pltpu.VMEM((4, experts, rows), F32),
                pltpu.VMEM((4 * rows, 128), F32),
                pltpu.VMEM((2, 2, n_own, hidden, ff), BF16),
                pltpu.VMEM((2, 2, n_own, hidden, ff), BF16),
                pltpu.VMEM((2, 2, n_own, ff, hidden), BF16),
                pltpu.VMEM((2, n_own, 4 * rows, ff), BF16),
                pltpu.VMEM((4 * rows, hidden), F32),
                pltpu.VMEM((rows, hidden), F32),
                pltpu.VMEM((rows, hidden), F32),
                pltpu.VMEM((rows, hidden), F32),
                dma((5,)), dma((8,)), dma((8,)),
                dma((n_own, 3)), dma((n_own, 3)),
                dma((n_own // 2, 3)), dma((n_own, 3)), dma((n_own // 2, 3)),
                dma((n_own, 3)), dma((n_own, 3)),
                dma((3, CHUNKS)), dma((3, CHUNKS)),
            ],
            compiler_params=pltpu.CompilerParams(
                collective_id=0, has_side_effects=True, vmem_limit_bytes=66_060_288
            ),
        )(tokens, gate_of, w_gate, w_up, w_down)

    return jax.shard_map(local_layer, mesh=mesh, in_specs=(row_spec, row_spec, row_spec, P("ep", None, "tp"), P("ep", None, "tp"), P("ep", "tp", None)), out_specs=row_spec, check_vma=False)
```

```python
import functools

import jax
import jax.numpy as jnp
from jax import lax
from jax.experimental import pallas as pl
from jax.experimental.pallas import tpu as pltpu
from jax.sharding import PartitionSpec as P

MESH = pl.DeviceIdType.MESH
F32 = jnp.float32
BF16 = jnp.bfloat16

CHUNKS = 8
NEAR_CHUNKS = 6


def layer_kernel(
    tok_h, ids_ref, gates_ref, wg_h, wu_h, wd_h, out_ref,
    tok, gtb, gm, wg, wu, wd, hid, acc, got_a, got_b, got_c,
    loc_sem, tok_ss, tok_rs, own_ss, own_rs, z_ss, q_rs, x_ss, c_ss, c_rs, out_ss, out_rs,
):
    n_own, hidden, ff = wg_h.shape
    half = n_own // 2
    rows = tok_h.shape[0]
    chunks = CHUNKS
    chunk = rows // chunks
    near = NEAR_CHUNKS
    part_at = (0, near * chunk)
    part_rows = (near * chunk, rows - near * chunk)
    x = lax.axis_index("dp")
    z = lax.axis_index("tp")
    ep = lax.axis_index("ep")
    core = lax.rem(ep, 2)
    to_x = {"dp": 1 - x}
    to_y = {"ep": lax.rem(ep + 2, 4)}
    to_c = {"ep": ep + 1 - 2 * core}
    to_z = {"tp": z + 1 - 2 * lax.rem(z, 2)}
    to_zz = {"tp": lax.rem(z + 2, 4)}
    row_d, row_c, row_b, row_a = 0, rows, 2 * rows, 3 * rows

    def rcopy(src, dst, ss, rs, dev):
        return pltpu.make_async_remote_copy(
            src_ref=src, dst_ref=dst, send_sem=ss, recv_sem=rs, device_id=dev, device_id_type=MESH
        )

    bufs = (wg, wu, wd)
    hbm = (wg_h, wu_h, wd_h)

    loc = [
        pltpu.make_async_copy(tok_h, tok.at[pl.ds(row_d, rows)], loc_sem.at[0]),
    ] + [pltpu.make_async_copy(hbm[a], bufs[a].at[0, 0], loc_sem.at[1 + a]) for a in range(3)]
    for cp in loc:
        cp.start()
    name = lax.broadcasted_iota(jnp.int32, (gtb.shape[1], rows), 0)
    mine_of = jnp.zeros(name.shape, F32)
    for j in range(ids_ref.shape[0]):
        mine_of += jnp.where(name == ids_ref[j : j + 1, :], gates_ref[j : j + 1, :], 0.0)
    gtb[0] = mine_of

    barrier = pltpu.get_barrier_semaphore()
    for dev in (to_x, to_y, to_c, to_z, to_zz):
        pl.semaphore_signal(barrier, inc=1, device_id=dev, device_id_type=MESH)
    with jax.named_scope("entry"):
        pl.semaphore_wait(barrier, 5)

    def part(base, p):
        return pl.ds(base + part_at[p], part_rows[p])

    tok_y = [rcopy(tok_h, tok.at[pl.ds(row_c, rows)], tok_ss.at[0], tok_rs.at[0], to_y)]
    gat_y = rcopy(gtb.at[0], gtb.at[1], tok_ss.at[1], tok_rs.at[1], to_y)
    gat_z = rcopy(gtb.at[0], gtb.at[2], tok_ss.at[2], tok_rs.at[2], to_zz)
    gat_f = rcopy(gtb.at[2], gtb.at[3], tok_ss.at[3], tok_rs.at[3], to_y)
    tok_z = [rcopy(tok_h.at[part(0, p)], tok.at[part(row_b, p)], tok_ss.at[4 + p], tok_rs.at[4 + p], to_zz)
             for p in range(2)]
    tok_f = [rcopy(tok.at[part(row_b, p)], tok.at[part(row_a, p)], tok_ss.at[6 + p], tok_rs.at[6 + p], to_y)
             for p in range(2)]

    def own_c(i, a):
        return rcopy(hbm[a].at[i], bufs[a].at[0, 1, i], own_ss.at[i, a], own_rs.at[i, a], to_c)

    def over_z(i, a):
        return rcopy(hbm[a].at[x * half + i], bufs[a].at[1, 0, 2 * i], z_ss.at[i, a], q_rs.at[2 * i, a], to_z)

    def over_x(i, a):
        return rcopy(bufs[a].at[1, 0, 2 * i], bufs[a].at[1, 0, 2 * i + 1], x_ss.at[i, a], q_rs.at[2 * i + 1, a], to_x)

    def over_c(q, a):
        return rcopy(bufs[a].at[1, 0, q], bufs[a].at[1, 1, q], c_ss.at[q, a], c_rs.at[q, a], to_c)

    tok_z[0].start()
    tok_y[0].start()
    gat_z.start()
    gat_y.start()
    for a in range(3):
        own_c(0, a).start()
    for i in range(half):
        for a in range(3):
            over_z(i, a).start()
    for i in range(1, n_own):
        for a in range(3):
            own_c(i, a).start()

    def zero(t, carry):
        acc[pl.ds(pl.multiple_of(t * rows, rows), rows)] = jnp.zeros((rows, hidden), F32)
        return carry

    lax.fori_loop(0, 4, zero, 0)

    def gates_of(b):
        block = gtb[b]
        full = jnp.concatenate([block, jnp.zeros((128 - block.shape[0], rows), F32)], axis=0)
        gm[pl.ds(b * rows, rows)] = full.T

    with jax.named_scope("loc"):
        for cp in loc:
            cp.wait()
    gates_of(0)

    base = (ep * n_own, (ep + 1 - 2 * core) * n_own)
    cols = min(256, hidden)

    def inner(xb, s, c, i):
        w_in = jnp.concatenate([wg[s, c, i], wu[s, c, i]], axis=1)
        both = jnp.dot(xb, w_in, preferred_element_type=F32)
        return (jax.nn.silu(both[:, :ff]) * both[:, ff:]).astype(BF16)

    def first(r, m, i):
        at = pl.ds(r, m)
        xb = tok[at]
        for c in range(2):
            hid[c, i, at] = inner(xb, 0, c, i)

    def second(r, m, q):
        at = pl.ds(r, m)
        i = ((x + q) % 2) * half + q // 2
        xb = tok[at]
        gates = gm[at]
        lane = lax.broadcasted_iota(jnp.int32, (m, 128), 1)
        hs, gs = [], []
        for c in range(2):
            hs.append(jnp.concatenate([hid[c, i, at], inner(xb, 1, c, q)], axis=1))
            gs.append(jnp.sum(jnp.where(lane == base[c] + i, gates, 0.0), axis=1, keepdims=True))
        for t in range(hidden // cols):
            sl = pl.ds(t * cols, cols)
            total = acc[at, sl]
            for c in range(2):
                w_out = jnp.concatenate([wd[0, c, i, :, sl], wd[1, c, q, :, sl]], axis=0)
                total += gs[c] * jnp.dot(hs[c], w_out, preferred_element_type=F32)
            acc[at, sl] = total

    def first_all(r, m):
        def go(i, carry):
            first(r, m, i)
            return carry

        lax.fori_loop(0, n_own, go, 0)

    def second_all(r, m):
        def go(q, carry):
            second(r, m, q)
            return carry

        lax.fori_loop(0, n_own, go, 0)

    def pass_z(n):
        u, a = n // 3, n % 3
        with jax.named_scope(f"ev_z{n}"):
            over_z(u, a).wait_recv()
        over_x(u, a).start()
        over_c(2 * u, a).start()

    def pass_x(u):
        with jax.named_scope(f"ev_x{u}"):
            for a in range(3):
                over_x(u, a).wait_recv()
                over_c(2 * u + 1, a).start()

    def rows_of(j):
        return pl.ds(j * chunk, chunk)

    def send_a(j):
        return rcopy(acc.at[pl.ds(row_a + j * chunk, chunk)], got_a.at[rows_of(j)], out_ss.at[0, j], out_rs.at[0, j], to_y)

    def send_b(j):
        return rcopy(acc.at[pl.ds(row_b + j * chunk, chunk)], got_b.at[rows_of(j)], out_ss.at[1, j], out_rs.at[1, j], to_zz)

    def send_c(j):
        return rcopy(acc.at[pl.ds(row_c + j * chunk, chunk)], got_c.at[rows_of(j)], out_ss.at[2, j], out_rs.at[2, j], to_y)

    def add_a(j):
        with jax.named_scope(f"late_a{j}"):
            send_a(j).wait_recv()
        at = pl.ds(row_b + j * chunk, chunk)
        acc[at] = acc[at] + got_a[rows_of(j)]
        send_b(j).start()

    def mine(i, carry):
        with jax.named_scope("ev_own"):
            for a in range(3):
                own_c(i, a).wait_recv()
        first(row_d, rows, i)
        return carry

    lax.fori_loop(0, n_own, mine, 0)

    pass_z(0)
    with jax.named_scope("ev_tok_c"):
        tok_y[0].wait_recv()
        gat_y.wait_recv()
    gates_of(1)
    first_all(row_c, rows)
    pass_z(1)
    with jax.named_scope("ev_tok_b1"):
        tok_z[0].wait_recv()
        gat_z.wait_recv()
    tok_f[0].start()
    gat_f.start()
    gates_of(2)
    pass_z(2)
    first_all(row_b, part_rows[0])
    pass_z(3)

    inner_layer = lax.rem(z * (3 - z), 3) // 2

    def events(q, table):
        for at, ns, us in table:
            @pl.when(q == at)
            def _(ns=ns, us=us):
                for n in ns:
                    pass_z(n)
                for u in us:
                    pass_x(u)

    def step(q, carry):
        events(q, ((1, (4,), (0,)), (2, (5,), ()), (3, (7,), (1,)), (4, (8,), ()), (5, (9,), (2,)),
                   (6, (11,), ()), (7, (), (3,))))

        @pl.when(q == 5 + inner_layer)
        def _():
            tok_z[1].start()

        with jax.named_scope("ev_q"):
            for a in range(3):
                over_c(q, a).wait_recv()

        @pl.when(q == 2)
        def _():
            with jax.named_scope("ev_tok_a1"):
                tok_f[0].wait_recv()
                gat_f.wait_recv()
            gates_of(3)
            first_all(row_a, part_rows[0])

            def go(p, carry):
                second(row_a, part_rows[0], p)
                return carry

            lax.fori_loop(0, 2, go, 0)

        @pl.when(q >= 2)
        def _():
            second(row_a, part_rows[0], q)

        @pl.when(q == n_own - 1)
        def _():
            with jax.named_scope("out_a1"):
                for j in range(near // 2):
                    send_a(j).start()

        events(q, ((2, (6,), ()), (5, (10,), ())))
        second(row_b, part_rows[0], q)
        second(row_c, rows, q)
        second(row_d, rows, q)
        return carry

    lax.fori_loop(0, n_own, step, 0)

    with jax.named_scope("ev_tok_b2"):
        tok_z[1].wait_recv()
    tok_f[1].start()
    for j in range(near // 2, near):
        send_a(j).start()
    add_a(0)
    first_all(row_b + part_at[1], part_rows[1])
    second_all(row_b + part_at[1], part_rows[1])
    add_a(1)
    add_a(2)
    with jax.named_scope("ev_tok_a2"):
        tok_f[1].wait_recv()
    first_all(row_a + part_at[1], part_rows[1])
    second_all(row_a + part_at[1], part_rows[1])
    with jax.named_scope("out_a2"):
        for j in range(near, chunks):
            send_a(j).start()
    for j in range(chunks):
        send_c(j).start()
    for j in range(3, chunks):
        add_a(j)
    for j in range(chunks):
        with jax.named_scope(f"late_b{j}"):
            send_b(j).wait_recv()
        with jax.named_scope(f"late_c{j}"):
            send_c(j).wait_recv()
        out_ref[rows_of(j)] = (acc[rows_of(j)] + got_c[rows_of(j)] + got_b[rows_of(j)]).astype(out_ref.dtype)

    for cp in tok_y + tok_z + tok_f + [gat_y, gat_z, gat_f]:
        cp.wait_send()
    for a in range(3):
        for i in range(n_own):
            own_c(i, a).wait_send()
            over_c(i, a).wait_send()
        for i in range(half):
            over_z(i, a).wait_send()
            over_x(i, a).wait_send()
    for j in range(chunks):
        send_a(j).wait_send()
        send_b(j).wait_send()
        send_c(j).wait_send()


def solution(mesh):
    row_spec = P(("dp", "ep", "tp"), None)

    def local_layer(tokens, expert_ids, gates, w_gate, w_up, w_down):
        n_own = w_gate.shape[0]
        rows, hidden = tokens.shape
        ff = w_gate.shape[2]
        experts = n_own * mesh.shape["ep"]
        any_spec = pl.BlockSpec(memory_space=pl.ANY)
        vmem_spec = pl.BlockSpec(memory_space=pltpu.VMEM)
        dma = pltpu.SemaphoreType.DMA
        return pl.pallas_call(
            layer_kernel,
            out_shape=jax.ShapeDtypeStruct((rows, hidden), jnp.bfloat16),
            in_specs=[any_spec, vmem_spec, vmem_spec, any_spec, any_spec, any_spec],
            out_specs=vmem_spec,
            scratch_shapes=[
                pltpu.VMEM((4 * rows, hidden), BF16),
                pltpu.VMEM((4, experts, rows), F32),
                pltpu.VMEM((4 * rows, 128), F32),
                pltpu.VMEM((2, 2, n_own, hidden, ff), BF16),
                pltpu.VMEM((2, 2, n_own, hidden, ff), BF16),
                pltpu.VMEM((2, 2, n_own, ff, hidden), BF16),
                pltpu.VMEM((2, n_own, 4 * rows, ff), BF16),
                pltpu.VMEM((4 * rows, hidden), F32),
                pltpu.VMEM((rows, hidden), F32),
                pltpu.VMEM((rows, hidden), F32),
                pltpu.VMEM((rows, hidden), F32),
                dma((4,)), dma((8,)), dma((8,)),
                dma((n_own, 3)), dma((n_own, 3)),
                dma((n_own // 2, 3)), dma((n_own, 3)), dma((n_own // 2, 3)),
                dma((n_own, 3)), dma((n_own, 3)),
                dma((3, CHUNKS)), dma((3, CHUNKS)),
            ],
            compiler_params=pltpu.CompilerParams(
                collective_id=0, has_side_effects=True, vmem_limit_bytes=66_060_288
            ),
        )(tokens, expert_ids.T, gates.T, w_gate, w_up, w_down)

    return jax.shard_map(local_layer, mesh=mesh, in_specs=(row_spec, row_spec, row_spec, P("ep", None, "tp"), P("ep", None, "tp"), P("ep", "tp", None)), out_specs=row_spec, check_vma=False)
```

```python
import functools

import jax
import jax.numpy as jnp
from jax import lax
from jax.experimental import pallas as pl
from jax.experimental.pallas import tpu as pltpu
from jax.sharding import PartitionSpec as P

MESH = pl.DeviceIdType.MESH
F32 = jnp.float32
BF16 = jnp.bfloat16

CHUNKS = 16
NEAR_CHUNKS = 10


def layer_kernel(
    tok_h, ids_ref, gates_ref, wg_h, wu_h, wd_h, out_ref,
    tok, gtb, gm, wg, wu, wd, hid, acc, got_a, got_b, got_c,
    loc_sem, tok_ss, tok_rs, own_ss, own_rs, z_ss, q_rs, x_ss, c_ss, c_rs, out_ss, out_rs,
):
    n_own, hidden, ff = wg_h.shape
    half = n_own // 2
    rows = tok_h.shape[0]
    chunks = CHUNKS
    chunk = rows // chunks
    near = NEAR_CHUNKS
    part_at = (0, near * chunk)
    part_rows = (near * chunk, rows - near * chunk)
    x = lax.axis_index("dp")
    z = lax.axis_index("tp")
    ep = lax.axis_index("ep")
    core = lax.rem(ep, 2)
    to_x = {"dp": 1 - x}
    to_y = {"ep": lax.rem(ep + 2, 4)}
    to_c = {"ep": ep + 1 - 2 * core}
    to_z = {"tp": z + 1 - 2 * lax.rem(z, 2)}
    to_zz = {"tp": lax.rem(z + 2, 4)}
    row_d, row_c, row_b, row_a = 0, rows, 2 * rows, 3 * rows

    def rcopy(src, dst, ss, rs, dev):
        return pltpu.make_async_remote_copy(
            src_ref=src, dst_ref=dst, send_sem=ss, recv_sem=rs, device_id=dev, device_id_type=MESH
        )

    bufs = (wg, wu, wd)
    hbm = (wg_h, wu_h, wd_h)

    loc = [
        pltpu.make_async_copy(tok_h, tok.at[pl.ds(row_d, rows)], loc_sem.at[0]),
    ] + [pltpu.make_async_copy(hbm[a], bufs[a].at[0, 0], loc_sem.at[1 + a]) for a in range(3)]
    for cp in loc:
        cp.start()
    name = lax.broadcasted_iota(jnp.int32, (gtb.shape[1], rows), 0)
    mine_of = jnp.zeros(name.shape, F32)
    for j in range(ids_ref.shape[0]):
        mine_of += jnp.where(name == ids_ref[j : j + 1, :], gates_ref[j : j + 1, :], 0.0)
    gtb[0] = mine_of

    barrier = pltpu.get_barrier_semaphore()
    for dev in (to_x, to_y, to_c, to_z, to_zz):
        pl.semaphore_signal(barrier, inc=1, device_id=dev, device_id_type=MESH)
    with jax.named_scope("entry"):
        pl.semaphore_wait(barrier, 5)

    def part(base, p):
        return pl.ds(base + part_at[p], part_rows[p])

    tok_y = [rcopy(tok_h, tok.at[pl.ds(row_c, rows)], tok_ss.at[0], tok_rs.at[0], to_y)]
    gat_y = rcopy(gtb.at[0], gtb.at[1], tok_ss.at[1], tok_rs.at[1], to_y)
    gat_z = rcopy(gtb.at[0], gtb.at[2], tok_ss.at[2], tok_rs.at[2], to_zz)
    gat_f = rcopy(gtb.at[2], gtb.at[3], tok_ss.at[3], tok_rs.at[3], to_y)
    tok_z = [rcopy(tok_h.at[part(0, p)], tok.at[part(row_b, p)], tok_ss.at[4 + p], tok_rs.at[4 + p], to_zz)
             for p in range(2)]
    tok_f = [rcopy(tok.at[part(row_b, p)], tok.at[part(row_a, p)], tok_ss.at[6 + p], tok_rs.at[6 + p], to_y)
             for p in range(2)]

    def own_c(i, a):
        return rcopy(hbm[a].at[i], bufs[a].at[0, 1, i], own_ss.at[i, a], own_rs.at[i, a], to_c)

    def pieces(i):
        return [(a, p) for a in range(3) for p in range(2 if i == half - 1 else 1)]

    def piece(ref, i, p):
        if i < half - 1:
            return ref
        n = ref.shape[0] // 2
        return ref.at[pl.ds(p * n, n)]

    def over_z(i, a, p):
        return rcopy(piece(hbm[a].at[x * half + i], i, p), piece(bufs[a].at[1, 0, 2 * i], i, p),
                     z_ss.at[i, a, p], q_rs.at[2 * i, a, p], to_z)

    def over_x(i, a, p):
        return rcopy(piece(bufs[a].at[1, 0, 2 * i], i, p), piece(bufs[a].at[1, 0, 2 * i + 1], i, p),
                     x_ss.at[i, a, p], q_rs.at[2 * i + 1, a, p], to_x)

    def over_c(q, a, p):
        i = q // 2
        return rcopy(piece(bufs[a].at[1, 0, q], i, p), piece(bufs[a].at[1, 1, q], i, p),
                     c_ss.at[q, a, p], c_rs.at[q, a, p], to_c)

    tok_z[0].start()
    tok_y[0].start()
    gat_z.start()
    gat_y.start()
    for a in range(3):
        own_c(0, a).start()
    for i in range(half):
        for a, p in pieces(i):
            over_z(i, a, p).start()
    for i in range(1, n_own):
        for a in range(3):
            own_c(i, a).start()

    def zero(t, carry):
        acc[pl.ds(pl.multiple_of(t * rows, rows), rows)] = jnp.zeros((rows, hidden), F32)
        return carry

    lax.fori_loop(0, 4, zero, 0)

    def gates_of(b):
        block = gtb[b]
        full = jnp.concatenate([block, jnp.zeros((128 - block.shape[0], rows), F32)], axis=0)
        gm[pl.ds(b * rows, rows)] = full.T

    with jax.named_scope("loc"):
        for cp in loc:
            cp.wait()
    gates_of(0)

    base = (ep * n_own, (ep + 1 - 2 * core) * n_own)
    cols = min(256, hidden)

    def inner(xb, s, c, i):
        w_in = jnp.concatenate([wg[s, c, i], wu[s, c, i]], axis=1)
        both = jnp.dot(xb, w_in, preferred_element_type=F32)
        return (jax.nn.silu(both[:, :ff]) * both[:, ff:]).astype(BF16)

    def first(r, m, i):
        at = pl.ds(r, m)
        xb = tok[at]
        for c in range(2):
            hid[c, i, at] = inner(xb, 0, c, i)

    def second(r, m, q):
        at = pl.ds(r, m)
        i = ((x + q) % 2) * half + q // 2
        xb = tok[at]
        gates = gm[at]
        lane = lax.broadcasted_iota(jnp.int32, (m, 128), 1)
        hs, gs = [], []
        for c in range(2):
            hs.append(jnp.concatenate([hid[c, i, at], inner(xb, 1, c, q)], axis=1))
            gs.append(jnp.sum(jnp.where(lane == base[c] + i, gates, 0.0), axis=1, keepdims=True))
        for t in range(hidden // cols):
            sl = pl.ds(t * cols, cols)
            total = acc[at, sl]
            for c in range(2):
                w_out = jnp.concatenate([wd[0, c, i, :, sl], wd[1, c, q, :, sl]], axis=0)
                total += gs[c] * jnp.dot(hs[c], w_out, preferred_element_type=F32)
            acc[at, sl] = total

    z_list = [(i, a, p) for i in range(half) for a, p in pieces(i)]

    def pass_z(n):
        i, a, p = z_list[n]
        with jax.named_scope(f"ev_z{n}"):
            over_z(i, a, p).wait_recv()
        over_x(i, a, p).start()
        over_c(2 * i, a, p).start()

    def pass_x(i):
        with jax.named_scope(f"ev_x{i}"):
            for a, p in pieces(i):
                over_x(i, a, p).wait_recv()
                over_c(2 * i + 1, a, p).start()

    def wait_c(q):
        with jax.named_scope(f"ev_q{q}"):
            for a, p in pieces(q // 2):
                over_c(q, a, p).wait_recv()

    def rows_of(j):
        return pl.ds(j * chunk, chunk)

    def send_a(j):
        return rcopy(acc.at[pl.ds(row_a + j * chunk, chunk)], got_a.at[rows_of(j)], out_ss.at[0, j], out_rs.at[0, j], to_y)

    def send_b(j):
        return rcopy(acc.at[pl.ds(row_b + j * chunk, chunk)], got_b.at[rows_of(j)], out_ss.at[1, j], out_rs.at[1, j], to_zz)

    def send_c(j):
        return rcopy(acc.at[pl.ds(row_c + j * chunk, chunk)], got_c.at[rows_of(j)], out_ss.at[2, j], out_rs.at[2, j], to_y)

    def add_a(j):
        with jax.named_scope(f"late_a{j}"):
            send_a(j).wait_recv()
        at = pl.ds(row_b + j * chunk, chunk)
        acc[at] = acc[at] + got_a[rows_of(j)]
        send_b(j).start()

    def mine(i, carry):
        with jax.named_scope("ev_own"):
            for a in range(3):
                own_c(i, a).wait_recv()
        first(row_d, rows, i)
        return carry

    lax.fori_loop(0, n_own, mine, 0)

    inner_layer = lax.rem(z * (3 - z), 3) // 2
    m_far = part_rows[0]

    def some(fn, r, m, lo, hi):
        def go(i, carry):
            fn(r, m, i)
            return carry

        lax.fori_loop(lo, hi, go, 0)

    def far_b():
        with jax.named_scope("ev_tok_b1"):
            tok_z[0].wait_recv()
            gat_z.wait_recv()
        tok_f[0].start()
        gat_f.start()
        gates_of(2)
        pass_z(2)
        some(first, row_b, m_far, 0, n_own)
        pass_z(3)

    def far_a():
        pass_z(6)
        with jax.named_scope("ev_tok_a1"):
            tok_f[0].wait_recv()
            gat_f.wait_recv()
        gates_of(3)
        some(first, row_a, m_far, 0, n_own)
        pass_x(1)
        some(second, row_a, m_far, 0, 2)
        pass_z(7)

    def late_tokens():
        @pl.when(inner_layer == 0)
        def _():
            tok_z[1].start()

    todo = {
        (0, 0): lambda: wait_c(0),
        (1, 0): lambda: (pass_x(0), wait_c(1)),
        (1, 1): lambda: pass_z(4),
        (2, 0): lambda: (pass_z(5), wait_c(2)),
        (2, 3): far_a,
        (3, 0): lambda: wait_c(3),
        (3, 2): lambda: pass_z(8),
        (4, 0): lambda: wait_c(4),
        (4, 1): lambda: pass_z(9),
        (4, 3): lambda: pass_z(10),
        (5, 0): lambda: (pass_x(2), pass_z(11), wait_c(5), late_tokens()),
        (5, 2): lambda: pass_z(12),
    }

    def checks(q, place):
        for (at, where), fn in todo.items():
            if where == place:
                @pl.when(q == at)
                def _(fn=fn):
                    fn()

    pass_z(0)
    with jax.named_scope("ev_tok_c"):
        tok_y[0].wait_recv()
        gat_y.wait_recv()
    gates_of(1)
    some(first, row_c, rows, 0, n_own)
    pass_z(1)
    far_b()

    def step(q, carry):
        checks(q, 0)
        second(row_c, rows, q)
        checks(q, 1)
        second(row_d, rows, q)
        checks(q, 2)
        second(row_b, m_far, q)
        checks(q, 3)

        @pl.when(q >= 2)
        def _():
            second(row_a, m_far, q)

        return carry

    last = n_own - 2
    lax.fori_loop(0, last, step, 0)

    pass_z(13)
    pass_z(14)

    @pl.when(inner_layer == 1)
    def _():
        tok_z[1].start()

    wait_c(last)

    def finish(q, carry):
        @pl.when(q == last + 1)
        def _():
            pass_x(half - 1)
            wait_c(last + 1)

        second(row_a, m_far, q)
        return carry

    lax.fori_loop(last, n_own, finish, 0)
    with jax.named_scope("out_a1"):
        for j in range(near // 2):
            send_a(j).start()
    some(second, row_b, m_far, last, n_own)
    add_a(0)
    some(second, row_c, rows, last, n_own)
    add_a(1)
    some(second, row_d, rows, last, n_own)
    add_a(2)
    with jax.named_scope("ev_tok_b2"):
        tok_z[1].wait_recv()
    tok_f[1].start()
    for j in range(near // 2, near):
        send_a(j).start()
    some(first, row_b + part_at[1], part_rows[1], 0, n_own)
    add_a(3)
    some(second, row_b + part_at[1], part_rows[1], 0, n_own)
    add_a(4)
    with jax.named_scope("ev_tok_a2"):
        tok_f[1].wait_recv()
    some(first, row_a + part_at[1], part_rows[1], 0, n_own)
    add_a(5)
    some(second, row_a + part_at[1], part_rows[1], 0, n_own)
    with jax.named_scope("out_a2"):
        for j in range(near, chunks):
            send_a(j).start()
    for j in range(chunks):
        send_c(j).start()
    for j in range(6, chunks):
        add_a(j)
    for j in range(chunks):
        with jax.named_scope(f"late_b{j}"):
            send_b(j).wait_recv()
        with jax.named_scope(f"late_c{j}"):
            send_c(j).wait_recv()
        out_ref[rows_of(j)] = (acc[rows_of(j)] + got_c[rows_of(j)] + got_b[rows_of(j)]).astype(out_ref.dtype)

    for cp in tok_y + tok_z + tok_f + [gat_y, gat_z, gat_f]:
        cp.wait_send()
    for a in range(3):
        for i in range(n_own):
            own_c(i, a).wait_send()
    for i in range(half):
        for a, p in pieces(i):
            over_z(i, a, p).wait_send()
            over_x(i, a, p).wait_send()
            over_c(2 * i, a, p).wait_send()
            over_c(2 * i + 1, a, p).wait_send()
    for j in range(chunks):
        send_a(j).wait_send()
        send_b(j).wait_send()
        send_c(j).wait_send()


def solution(mesh):
    row_spec = P(("dp", "ep", "tp"), None)

    def local_layer(tokens, expert_ids, gates, w_gate, w_up, w_down):
        n_own = w_gate.shape[0]
        rows, hidden = tokens.shape
        ff = w_gate.shape[2]
        experts = n_own * mesh.shape["ep"]
        any_spec = pl.BlockSpec(memory_space=pl.ANY)
        vmem_spec = pl.BlockSpec(memory_space=pltpu.VMEM)
        dma = pltpu.SemaphoreType.DMA
        return pl.pallas_call(
            layer_kernel,
            out_shape=jax.ShapeDtypeStruct((rows, hidden), jnp.bfloat16),
            in_specs=[any_spec, vmem_spec, vmem_spec, any_spec, any_spec, any_spec],
            out_specs=vmem_spec,
            scratch_shapes=[
                pltpu.VMEM((4 * rows, hidden), BF16),
                pltpu.VMEM((4, experts, rows), F32),
                pltpu.VMEM((4 * rows, 128), F32),
                pltpu.VMEM((2, 2, n_own, hidden, ff), BF16),
                pltpu.VMEM((2, 2, n_own, hidden, ff), BF16),
                pltpu.VMEM((2, 2, n_own, ff, hidden), BF16),
                pltpu.VMEM((2, n_own, 4 * rows, ff), BF16),
                pltpu.VMEM((4 * rows, hidden), F32),
                pltpu.VMEM((rows, hidden), F32),
                pltpu.VMEM((rows, hidden), F32),
                pltpu.VMEM((rows, hidden), F32),
                dma((4,)), dma((8,)), dma((8,)),
                dma((n_own, 3)), dma((n_own, 3)),
                dma((n_own // 2, 3, 2)), dma((n_own, 3, 2)), dma((n_own // 2, 3, 2)),
                dma((n_own, 3, 2)), dma((n_own, 3, 2)),
                dma((3, CHUNKS)), dma((3, CHUNKS)),
            ],
            compiler_params=pltpu.CompilerParams(
                collective_id=0, has_side_effects=True, vmem_limit_bytes=66_060_288
            ),
        )(tokens, expert_ids.T, gates.T, w_gate, w_up, w_down)

    return jax.shard_map(local_layer, mesh=mesh, in_specs=(row_spec, row_spec, row_spec, P("ep", None, "tp"), P("ep", None, "tp"), P("ep", "tp", None)), out_specs=row_spec, check_vma=False)
```

```python
import functools

import jax
import jax.numpy as jnp
from jax import lax
from jax.experimental import pallas as pl
from jax.experimental.pallas import tpu as pltpu
from jax.sharding import PartitionSpec as P

MESH = pl.DeviceIdType.MESH
F32 = jnp.float32
BF16 = jnp.bfloat16

PIECES = 4
COLS = 256


def layer_kernel(
    tok_h, ids_ref, gates_ref, wg_h, wu_h, wd_h, out_ref,
    tok, raw, gm, wg, wu, wd, hid, acc, got_a, got_b, got_c,
    loc_sem, tok_ss, tok_rs, own_ss, own_rs, z_ss, z_rs, x_ss, x_rs, cz_ss, cz_rs, cx_ss, cx_rs, out_ss, out_rs,
):
    n_own, hidden, ff = wg_h.shape
    half = n_own // 2
    rows = tok_h.shape[0]
    part = rows // 2
    n_cols = hidden // COLS
    chunk = rows // PIECES
    top_k = ids_ref.shape[0]
    x = lax.axis_index("dp")
    z = lax.axis_index("tp")
    ep = lax.axis_index("ep")
    core = lax.rem(ep, 2)
    to_x = {"dp": 1 - x}
    to_y = {"ep": lax.rem(ep + 2, 4)}
    to_c = {"ep": ep + 1 - 2 * core}
    to_z = {"tp": z + 1 - 2 * lax.rem(z, 2)}
    to_zz = {"tp": lax.rem(z + 2, 4)}
    row_d, row_c, row_b, row_a = 0, rows, 2 * rows, 3 * rows

    def rcopy(src, dst, ss, rs, dev):
        return pltpu.make_async_remote_copy(
            src_ref=src, dst_ref=dst, send_sem=ss, recv_sem=rs, device_id=dev, device_id_type=MESH
        )

    bufs = (wg, wu, wd)
    hbm = (wg_h, wu_h, wd_h)

    loc = [pltpu.make_async_copy(tok_h, tok.at[pl.ds(row_d, rows)], loc_sem.at[0])]
    loc += [pltpu.make_async_copy(hbm[a], bufs[a].at[0, 0], loc_sem.at[1 + a]) for a in range(3)]
    for cp in loc:
        cp.start()
    raw[0, pl.ds(0, top_k)] = ids_ref[...].astype(F32)
    raw[0, pl.ds(top_k, top_k)] = gates_ref[...]

    barrier = pltpu.get_barrier_semaphore()
    for dev in (to_x, to_y, to_c, to_z, to_zz):
        pl.semaphore_signal(barrier, inc=1, device_id=dev, device_id_type=MESH)
    with jax.named_scope("entry"):
        pl.semaphore_wait(barrier, 5)

    def side(base, p):
        return pl.ds(base + p * part, part)

    tok_y = rcopy(tok_h, tok.at[pl.ds(row_c, rows)], tok_ss.at[0], tok_rs.at[0], to_y)
    gat_y = rcopy(raw.at[0], raw.at[1], tok_ss.at[1], tok_rs.at[1], to_y)
    gat_z = rcopy(raw.at[0], raw.at[2], tok_ss.at[2], tok_rs.at[2], to_zz)
    gat_f = rcopy(raw.at[2], raw.at[3], tok_ss.at[3], tok_rs.at[3], to_y)
    tok_z = [rcopy(tok_h.at[side(0, p)], tok.at[side(row_b, p)], tok_ss.at[4 + p], tok_rs.at[4 + p], to_zz)
             for p in range(2)]
    tok_f = [rcopy(tok.at[side(row_b, p)], tok.at[side(row_a, p)], tok_ss.at[6 + p], tok_rs.at[6 + p], to_y)
             for p in range(2)]

    def own_c(i, a):
        return rcopy(hbm[a].at[i], bufs[a].at[0, 1, i], own_ss.at[i, a], own_rs.at[i, a], to_c)

    n_in = 2 * half
    n_z = n_in + n_cols

    def at_slot(share, n, lo):
        if n < n_in:
            return bufs[n % 2].at[1, share, lo + n // 2]
        return wd.at[1, share, pl.ds(lo, half), :, pl.ds((n - n_in) * COLS, COLS)]

    def over_z(n):
        if n < n_in:
            src = hbm[n % 2].at[x * half + n // 2]
        else:
            src = wd_h.at[pl.ds(x * half, half), :, pl.ds((n - n_in) * COLS, COLS)]
        return rcopy(src, at_slot(0, n, 0), z_ss.at[n], z_rs.at[n], to_z)

    def over_x(n):
        return rcopy(at_slot(0, n, 0), at_slot(0, n, half), x_ss.at[n], x_rs.at[n], to_x)

    def over_cz(n):
        return rcopy(at_slot(0, n, 0), at_slot(1, n, 0), cz_ss.at[n], cz_rs.at[n], to_c)

    def over_cx(n):
        return rcopy(at_slot(0, n, half), at_slot(1, n, half), cx_ss.at[n], cx_rs.at[n], to_c)

    tok_z[0].start()
    tok_y.start()
    gat_z.start()
    gat_y.start()
    tok_z[1].start()
    for a in range(3):
        own_c(0, a).start()
    for n in range(n_z):
        over_z(n).start()
    for i in range(1, n_own):
        for a in range(3):
            own_c(i, a).start()

    base = (ep * n_own, (ep + 1 - 2 * core) * n_own)

    def gates_of(b):
        lane = lax.broadcasted_iota(jnp.int32, (2 * n_own, rows), 0)
        second_core = lane >= n_own
        t = jnp.where(second_core, lane - n_own, lane) + x * half
        t = jnp.where(t >= n_own, t - n_own, t)
        name = (t + jnp.where(second_core, base[1], base[0])).astype(F32)
        mine_of = jnp.zeros(name.shape, F32)
        for j in range(top_k):
            mine_of += jnp.where(name == raw[b, j : j + 1], raw[b, top_k + j : top_k + j + 1], 0.0)
        full = jnp.concatenate([mine_of, jnp.zeros((128 - 2 * n_own, rows), F32)], axis=0)
        gm[pl.ds(b * rows, rows)] = full.T

    with jax.named_scope("loc"):
        for cp in loc:
            cp.wait()
    gates_of(0)

    def slot(t):
        return (t % 2) * half + t // 2

    def inner(r, m, s, i):
        at = pl.ds(pl.multiple_of(r, m), m)
        xb = tok[at]
        for c in range(2):
            w_in = jnp.concatenate([wg[s, c, i], wu[s, c, i]], axis=1)
            both = jnp.dot(xb, w_in, preferred_element_type=F32)
            hid[s, c, i, at] = (jax.nn.silu(both[:, :ff]) * both[:, ff:]).astype(BF16)

    def first(r, m):
        def go(i, carry):
            inner(r, m, 0, i)
            return carry

        lax.fori_loop(0, n_own, go, 0)

    def second(r, m, lo, hi):
        def go(t, carry):
            inner(r, m, 1, slot(t))
            return carry

        lax.fori_loop(lo, hi, go, 0)

    def second_blocks(t, n):
        def go(b, carry):
            inner(b * rows, rows, 1, slot(t))
            return carry

        lax.fori_loop(0, n, go, 0)

    def down(r, k):
        at = pl.ds(r, rows)
        sl = pl.ds(pl.multiple_of(k * COLS, COLS), COLS)
        for q in range(n_own):
            i = lax.rem(x * half + q, n_own)
            total = None if q == 0 else acc[k, at]
            for c in range(2):
                h = jnp.concatenate([hid[0, c, i, at], hid[1, c, q, at]], axis=1)
                w_out = jnp.concatenate([wd[0, c, i, :, sl], wd[1, c, q, :, sl]], axis=0)
                lane = c * n_own + q
                term = gm[at, lane : lane + 1] * jnp.dot(h, w_out, preferred_element_type=F32)
                total = term if total is None else total + term
            acc[k, at] = total

    def pass_z(n):
        with jax.named_scope(f"ev_z{n}"):
            over_z(n).wait_recv()
        over_x(n).start()
        over_cz(n).start()

    def pass_x(n):
        with jax.named_scope(f"ev_x{n}"):
            over_x(n).wait_recv()
        over_cx(n).start()

    def ready(t):
        with jax.named_scope(f"ev_q{t}"):
            for n in (t - t % 2, t - t % 2 + 1):
                (over_cx(n) if t % 2 else over_cz(n)).wait_recv()

    def rows_of(j):
        return pl.ds(j * chunk, chunk)

    def out_copy(which, r, got, dev):
        def make(k, j):
            return rcopy(acc.at[k, pl.ds(r + j * chunk, chunk)], got.at[k, rows_of(j)],
                         out_ss.at[which, k, j], out_rs.at[which, k, j], dev)

        return make

    send_a = out_copy(0, row_a, got_a, to_y)
    send_b = out_copy(1, row_b, got_b, to_zz)
    send_c = out_copy(2, row_c, got_c, to_y)

    def add_a(k, j):
        with jax.named_scope(f"late_a{k}{j}"):
            send_a(k, j).wait_recv()
        at = pl.ds(row_b + j * chunk, chunk)
        acc[k, at] = acc[k, at] + got_a[k, rows_of(j)]
        send_b(k, j).start()

    def give(k, j):
        with jax.named_scope(f"late_c{k}{j}"):
            send_c(k, j).wait_recv()
        with jax.named_scope(f"late_b{k}{j}"):
            send_b(k, j).wait_recv()
        total = acc[k, rows_of(j)] + got_c[k, rows_of(j)] + got_b[k, rows_of(j)]
        out_ref[rows_of(j), pl.ds(k * COLS, COLS)] = total.astype(out_ref.dtype)

    def mine(i, carry):
        with jax.named_scope("ev_own"):
            for a in range(3):
                own_c(i, a).wait_recv()
        inner(row_d, rows, 0, i)
        return carry

    lax.fori_loop(0, n_own, mine, 0)

    with jax.named_scope("ev_tok_c"):
        tok_y.wait_recv()
        gat_y.wait_recv()
    gates_of(1)
    first(row_c, rows)
    pass_z(0)
    with jax.named_scope("ev_tok_b0"):
        tok_z[0].wait_recv()
        gat_z.wait_recv()
    tok_f[0].start()
    gat_f.start()
    gates_of(2)
    first(row_b, part)
    pass_z(1)
    with jax.named_scope("ev_tok_a0"):
        tok_f[0].wait_recv()
        gat_f.wait_recv()
    gates_of(3)
    first(row_a, part)
    pass_z(2)
    ready(0)
    second_blocks(0, 2)
    pass_x(0)
    pass_x(1)
    with jax.named_scope("ev_tok_b1"):
        tok_z[1].wait_recv()
    tok_f[1].start()
    pass_z(3)
    first(row_b + part, part)
    ready(1)
    second_blocks(1, 2)
    second(row_b, part, 0, 2)
    second(row_b + part, part, 0, 2)
    pass_z(4)
    ready(2)
    second_blocks(2, 3)
    pass_x(2)
    pass_x(3)
    second(row_a, part, 0, 3)
    pass_z(5)
    with jax.named_scope("ev_tok_a1"):
        tok_f[1].wait_recv()
    first(row_a + part, part)
    second(row_a + part, part, 0, 3)
    pass_z(6)
    ready(3)
    second_blocks(3, 4)
    pass_x(4)
    pass_x(5)
    ready(4)
    second_blocks(4, 4)
    pass_z(7)
    ready(5)
    second_blocks(5, 4)
    ready(6)
    second_blocks(6, 4)
    pass_z(8)
    pass_x(6)
    pass_x(7)
    ready(7)
    second_blocks(7, 4)
    pass_z(9)

    def column(k, carry):
        for m in range(n_cols):
            @pl.when(k == m)
            def _(m=m):
                n = n_in + m
                pass_x(n)
                with jax.named_scope(f"ev_w{m}"):
                    over_cz(n).wait_recv()
                    over_cx(n).wait_recv()

        down(row_a, k)
        with jax.named_scope("out_a"):
            for j in range(PIECES):
                send_a(k, j).start()

        @pl.when(k == 0)
        def _():
            pass_z(n_in + 2)

        @pl.when(k == 1)
        def _():
            add_a(0, 1)

        down(row_b, k)

        @pl.when(k == 0)
        def _():
            add_a(0, 0)
            pass_z(n_in + 3)

        @pl.when(k == 1)
        def _():
            add_a(0, 2)

        @pl.when(k == 2)
        def _():
            add_a(0, 3)

        down(row_c, k)
        for j in range(PIECES):
            send_c(k, j).start()
        down(row_d, k)
        return carry

    lax.fori_loop(0, n_cols, column, 0)
    for k in range(1, n_cols):
        for j in range(PIECES):
            add_a(k, j)
            give(k - 1, j)
    for j in range(PIECES):
        give(n_cols - 1, j)

    for cp in [tok_y, gat_y, gat_z, gat_f] + tok_z + tok_f:
        cp.wait_send()
    for a in range(3):
        for i in range(n_own):
            own_c(i, a).wait_send()
    for n in range(n_z):
        for cp in (over_z(n), over_x(n), over_cz(n), over_cx(n)):
            cp.wait_send()
    for k in range(n_cols):
        for j in range(PIECES):
            for cp in (send_a(k, j), send_b(k, j), send_c(k, j)):
                cp.wait_send()


def solution(mesh):
    row_spec = P(("dp", "ep", "tp"), None)

    def local_layer(tokens, expert_ids, gates, w_gate, w_up, w_down):
        n_own = w_gate.shape[0]
        rows, hidden = tokens.shape
        ff = w_gate.shape[2]
        n_cols = hidden // COLS
        n_z = n_own + n_cols
        any_spec = pl.BlockSpec(memory_space=pl.ANY)
        vmem_spec = pl.BlockSpec(memory_space=pltpu.VMEM)
        dma = pltpu.SemaphoreType.DMA
        return pl.pallas_call(
            layer_kernel,
            out_shape=jax.ShapeDtypeStruct((rows, hidden), jnp.bfloat16),
            in_specs=[any_spec, vmem_spec, vmem_spec, any_spec, any_spec, any_spec],
            out_specs=vmem_spec,
            scratch_shapes=[
                pltpu.VMEM((4 * rows, hidden), BF16),
                pltpu.VMEM((4, 2 * expert_ids.shape[1], rows), F32),
                pltpu.VMEM((4 * rows, 128), F32),
                pltpu.VMEM((2, 2, n_own, hidden, ff), BF16),
                pltpu.VMEM((2, 2, n_own, hidden, ff), BF16),
                pltpu.VMEM((2, 2, n_own, ff, hidden), BF16),
                pltpu.VMEM((2, 2, n_own, 4 * rows, ff), BF16),
                pltpu.VMEM((n_cols, 4 * rows, COLS), F32),
                pltpu.VMEM((n_cols, rows, COLS), F32),
                pltpu.VMEM((n_cols, rows, COLS), F32),
                pltpu.VMEM((n_cols, rows, COLS), F32),
                dma((4,)), dma((8,)), dma((8,)),
                dma((n_own, 3)), dma((n_own, 3)),
                dma((n_z,)), dma((n_z,)), dma((n_z,)), dma((n_z,)),
                dma((n_z,)), dma((n_z,)), dma((n_z,)), dma((n_z,)),
                dma((3, n_cols, PIECES)), dma((3, n_cols, PIECES)),
            ],
            compiler_params=pltpu.CompilerParams(
                collective_id=0, has_side_effects=True, vmem_limit_bytes=67_043_328
            ),
        )(tokens, expert_ids.T, gates.T, w_gate, w_up, w_down)

    return jax.shard_map(local_layer, mesh=mesh, in_specs=(row_spec, row_spec, row_spec, P("ep", None, "tp"), P("ep", None, "tp"), P("ep", "tp", None)), out_specs=row_spec, check_vma=False)
```

```python
import functools

import jax
import jax.numpy as jnp
from jax import lax
from jax.experimental import pallas as pl
from jax.experimental.pallas import tpu as pltpu
from jax.sharding import PartitionSpec as P

MESH = pl.DeviceIdType.MESH
F32 = jnp.float32
BF16 = jnp.bfloat16

PIECES = 4
COLS = 256


def layer_kernel(
    tok_h, ids_ref, gates_ref, wg_h, wu_h, wd_h, out_ref,
    tok, raw, gm, wg, wu, wd, hid, acc, got_a, got_b, got_c,
    loc_sem, tok_ss, tok_rs, own_ss, own_rs, z_ss, z_rs, x_ss, x_rs, cz_ss, cz_rs, cx_ss, cx_rs, out_ss, out_rs,
):
    n_own, hidden, ff = wg_h.shape
    half = n_own // 2
    rows = tok_h.shape[0]
    part = rows // 2
    n_cols = hidden // COLS
    chunk = rows // PIECES
    top_k = ids_ref.shape[0]
    x = lax.axis_index("dp")
    z = lax.axis_index("tp")
    ep = lax.axis_index("ep")
    core = lax.rem(ep, 2)
    to_x = {"dp": 1 - x}
    to_y = {"ep": lax.rem(ep + 2, 4)}
    to_c = {"ep": ep + 1 - 2 * core}
    to_z = {"tp": z + 1 - 2 * lax.rem(z, 2)}
    to_zz = {"tp": lax.rem(z + 2, 4)}
    row_d, row_c, row_b, row_a = 0, rows, 2 * rows, 3 * rows

    def rcopy(src, dst, ss, rs, dev):
        return pltpu.make_async_remote_copy(
            src_ref=src, dst_ref=dst, send_sem=ss, recv_sem=rs, device_id=dev, device_id_type=MESH
        )

    bufs = (wg, wu, wd)
    hbm = (wg_h, wu_h, wd_h)

    loc = [pltpu.make_async_copy(tok_h, tok.at[pl.ds(row_d, rows)], loc_sem.at[0])]
    loc += [pltpu.make_async_copy(hbm[a], bufs[a].at[0, 0], loc_sem.at[1 + a]) for a in range(3)]
    for cp in loc:
        cp.start()
    raw[0, pl.ds(0, top_k)] = ids_ref[...].astype(F32)
    raw[0, pl.ds(top_k, top_k)] = gates_ref[...]

    barrier = pltpu.get_barrier_semaphore()
    for dev in (to_x, to_y, to_c, to_z, to_zz):
        pl.semaphore_signal(barrier, inc=1, device_id=dev, device_id_type=MESH)
    with jax.named_scope("entry"):
        pl.semaphore_wait(barrier, 5)

    def side(base, p):
        return pl.ds(base + p * part, part)

    tok_y = [rcopy(tok_h.at[side(0, p)], tok.at[side(row_c, p)], tok_ss.at[8 * p], tok_rs.at[8 * p], to_y)
             for p in range(2)]
    gat_y = rcopy(raw.at[0], raw.at[1], tok_ss.at[1], tok_rs.at[1], to_y)
    gat_z = rcopy(raw.at[0], raw.at[2], tok_ss.at[2], tok_rs.at[2], to_zz)
    gat_f = rcopy(raw.at[2], raw.at[3], tok_ss.at[3], tok_rs.at[3], to_y)
    tok_z = [rcopy(tok_h.at[side(0, p)], tok.at[side(row_b, p)], tok_ss.at[4 + p], tok_rs.at[4 + p], to_zz)
             for p in range(2)]
    tok_f = [rcopy(tok.at[side(row_b, p)], tok.at[side(row_a, p)], tok_ss.at[6 + p], tok_rs.at[6 + p], to_y)
             for p in range(2)]

    def own_c(i, a):
        return rcopy(hbm[a].at[i], bufs[a].at[0, 1, i], own_ss.at[i, a], own_rs.at[i, a], to_c)

    n_in = 2 * half
    n_z = n_in + n_cols

    def at_slot(share, n, lo):
        if n < n_in:
            return bufs[n % 2].at[1, share, lo + n // 2]
        return wd.at[1, share, pl.ds(lo, half), :, pl.ds((n - n_in) * COLS, COLS)]

    def over_z(n):
        if n < n_in:
            src = hbm[n % 2].at[x * half + n // 2]
        else:
            src = wd_h.at[pl.ds(x * half, half), :, pl.ds((n - n_in) * COLS, COLS)]
        return rcopy(src, at_slot(0, n, 0), z_ss.at[n], z_rs.at[n], to_z)

    def over_x(n):
        return rcopy(at_slot(0, n, 0), at_slot(0, n, half), x_ss.at[n], x_rs.at[n], to_x)

    def over_cz(n):
        return rcopy(at_slot(0, n, 0), at_slot(1, n, 0), cz_ss.at[n], cz_rs.at[n], to_c)

    def over_cx(n):
        return rcopy(at_slot(0, n, half), at_slot(1, n, half), cx_ss.at[n], cx_rs.at[n], to_c)

    inner_layer = lax.rem(z * (3 - z), 3) // 2
    tok_z[0].start()
    tok_y[0].start()
    gat_z.start()
    gat_y.start()
    tok_y[1].start()

    @pl.when(inner_layer == 0)
    def _():
        tok_z[1].start()

    for a in range(3):
        own_c(0, a).start()
    for n in range(n_z):
        over_z(n).start()
    for i in range(1, n_own):
        for a in range(3):
            own_c(i, a).start()

    base = (ep * n_own, (ep + 1 - 2 * core) * n_own)

    def gates_of(b):
        lane = lax.broadcasted_iota(jnp.int32, (2 * n_own, rows), 0)
        second_core = lane >= n_own
        t = jnp.where(second_core, lane - n_own, lane) + x * half
        t = jnp.where(t >= n_own, t - n_own, t)
        name = (t + jnp.where(second_core, base[1], base[0])).astype(F32)
        mine_of = jnp.zeros(name.shape, F32)
        for j in range(top_k):
            mine_of += jnp.where(name == raw[b, j : j + 1], raw[b, top_k + j : top_k + j + 1], 0.0)
        full = jnp.concatenate([mine_of, jnp.zeros((128 - 2 * n_own, rows), F32)], axis=0)
        gm[pl.ds(b * rows, rows)] = full.T

    with jax.named_scope("loc"):
        for cp in loc:
            cp.wait()
    gates_of(0)

    def slot(t):
        return (t % 2) * half + t // 2

    def inner(r, m, s, i):
        at = pl.ds(pl.multiple_of(r, m), m)
        xb = tok[at]
        for c in range(2):
            w_in = jnp.concatenate([wg[s, c, i], wu[s, c, i]], axis=1)
            both = jnp.dot(xb, w_in, preferred_element_type=F32)
            hid[s, c, i, at] = (jax.nn.silu(both[:, :ff]) * both[:, ff:]).astype(BF16)

    def first(r, m):
        def go(i, carry):
            inner(r, m, 0, i)
            return carry

        lax.fori_loop(0, n_own, go, 0)

    def second(r, m, lo, hi):
        def go(t, carry):
            inner(r, m, 1, slot(t))
            return carry

        lax.fori_loop(lo, hi, go, 0)

    def second_blocks(t, lo, hi):
        def go(b, carry):
            inner(b * rows, rows, 1, slot(t))
            return carry

        lax.fori_loop(lo, hi, go, 0)

    def down(r, k):
        at = pl.ds(r, rows)
        sl = pl.ds(pl.multiple_of(k * COLS, COLS), COLS)
        for q in range(n_own):
            i = lax.rem(x * half + q, n_own)
            total = None if q == 0 else acc[k, at]
            for c in range(2):
                h = jnp.concatenate([hid[0, c, i, at], hid[1, c, q, at]], axis=1)
                w_out = jnp.concatenate([wd[0, c, i, :, sl], wd[1, c, q, :, sl]], axis=0)
                lane = c * n_own + q
                term = gm[at, lane : lane + 1] * jnp.dot(h, w_out, preferred_element_type=F32)
                total = term if total is None else total + term
            acc[k, at] = total

    def pass_z(n):
        with jax.named_scope(f"ev_z{n}"):
            over_z(n).wait_recv()
        over_x(n).start()
        over_cz(n).start()

    def pass_x(n):
        with jax.named_scope(f"ev_x{n}"):
            over_x(n).wait_recv()
        over_cx(n).start()

    def ready(t):
        with jax.named_scope(f"ev_q{t}"):
            for n in (t - t % 2, t - t % 2 + 1):
                (over_cx(n) if t % 2 else over_cz(n)).wait_recv()

    def rows_of(j):
        return pl.ds(j * chunk, chunk)

    def out_copy(which, r, got, dev):
        def make(k, j):
            return rcopy(acc.at[k, pl.ds(r + j * chunk, chunk)], got.at[k, rows_of(j)],
                         out_ss.at[which, k, j], out_rs.at[which, k, j], dev)

        return make

    send_a = out_copy(0, row_a, got_a, to_y)
    send_b = out_copy(1, row_b, got_b, to_zz)
    send_c = out_copy(2, row_c, got_c, to_y)

    def add_a(k, j):
        with jax.named_scope(f"late_a{k}{j}"):
            send_a(k, j).wait_recv()
        at = pl.ds(row_b + j * chunk, chunk)
        acc[k, at] = acc[k, at] + got_a[k, rows_of(j)]
        send_b(k, j).start()

    def give(k, j):
        with jax.named_scope(f"late_c{k}{j}"):
            send_c(k, j).wait_recv()
        with jax.named_scope(f"late_b{k}{j}"):
            send_b(k, j).wait_recv()
        total = acc[k, rows_of(j)] + got_c[k, rows_of(j)] + got_b[k, rows_of(j)]
        out_ref[rows_of(j), pl.ds(k * COLS, COLS)] = total.astype(out_ref.dtype)

    def mine(i, carry):
        with jax.named_scope("ev_own"):
            for a in range(3):
                own_c(i, a).wait_recv()
        inner(row_d, rows, 0, i)
        return carry

    lax.fori_loop(0, n_own, mine, 0)

    @pl.when(inner_layer == 1)
    def _():
        tok_z[1].start()

    with jax.named_scope("ev_tok_c0"):
        tok_y[0].wait_recv()
        gat_y.wait_recv()
    gates_of(1)
    first(row_c, part)
    with jax.named_scope("ev_tok_c1"):
        tok_y[1].wait_recv()
    first(row_c + part, part)
    with jax.named_scope("ev_tok_b0"):
        tok_z[0].wait_recv()
        gat_z.wait_recv()
    tok_f[0].start()
    gat_f.start()
    pass_z(0)
    gates_of(2)
    first(row_b, part)
    pass_z(1)
    ready(0)
    second_blocks(0, 0, 2)
    second(row_b, part, 0, 1)
    pass_z(2)
    with jax.named_scope("ev_tok_a0"):
        tok_f[0].wait_recv()
        gat_f.wait_recv()
    gates_of(3)
    first(row_a, part)
    pass_x(0)
    pass_x(1)
    with jax.named_scope("ev_tok_b1"):
        tok_z[1].wait_recv()
    tok_f[1].start()
    pass_z(3)
    first(row_b + part, part)
    ready(1)
    second_blocks(1, 0, 2)
    second(row_b, part, 1, 2)
    second(row_b + part, part, 0, 2)
    pass_z(4)
    ready(2)
    second_blocks(2, 0, 3)
    pass_x(2)
    pass_x(3)
    second(row_a, part, 0, 3)
    pass_z(5)
    with jax.named_scope("ev_tok_a1"):
        tok_f[1].wait_recv()
    first(row_a + part, part)
    second(row_a + part, part, 0, 3)
    ready(3)
    second_blocks(3, 0, 2)
    pass_z(6)
    second_blocks(3, 2, 4)
    pass_x(4)
    pass_x(5)
    ready(4)
    second_blocks(4, 0, 4)
    pass_z(7)
    ready(5)
    second_blocks(5, 0, 4)
    ready(6)
    second_blocks(6, 0, 4)
    pass_z(8)
    pass_x(6)
    pass_x(7)
    ready(7)
    second_blocks(7, 0, 4)
    pass_z(9)

    def column(k, carry):
        for m in range(n_cols):
            @pl.when(k == m)
            def _(m=m):
                n = n_in + m
                pass_x(n)
                with jax.named_scope(f"ev_w{m}"):
                    over_cz(n).wait_recv()
                    over_cx(n).wait_recv()

        down(row_a, k)
        with jax.named_scope("out_a"):
            for j in range(PIECES):
                send_a(k, j).start()

        @pl.when(k == 0)
        def _():
            pass_z(n_in + 2)

        @pl.when(k == 1)
        def _():
            add_a(0, 1)

        down(row_b, k)

        @pl.when(k == 0)
        def _():
            add_a(0, 0)
            pass_z(n_in + 3)

        @pl.when(k == 1)
        def _():
            add_a(0, 2)

        @pl.when(k == 2)
        def _():
            add_a(0, 3)

        down(row_c, k)
        for j in range(PIECES):
            send_c(k, j).start()
        down(row_d, k)
        return carry

    lax.fori_loop(0, n_cols, column, 0)
    for k in range(1, n_cols):
        for j in range(PIECES):
            add_a(k, j)
            give(k - 1, j)
    for j in range(PIECES):
        give(n_cols - 1, j)

    for cp in [gat_y, gat_z, gat_f] + tok_y + tok_z + tok_f:
        cp.wait_send()
    for a in range(3):
        for i in range(n_own):
            own_c(i, a).wait_send()
    for n in range(n_z):
        for cp in (over_z(n), over_x(n), over_cz(n), over_cx(n)):
            cp.wait_send()
    for k in range(n_cols):
        for j in range(PIECES):
            for cp in (send_a(k, j), send_b(k, j), send_c(k, j)):
                cp.wait_send()


def solution(mesh):
    row_spec = P(("dp", "ep", "tp"), None)

    def local_layer(tokens, expert_ids, gates, w_gate, w_up, w_down):
        n_own = w_gate.shape[0]
        rows, hidden = tokens.shape
        ff = w_gate.shape[2]
        n_cols = hidden // COLS
        n_z = n_own + n_cols
        any_spec = pl.BlockSpec(memory_space=pl.ANY)
        vmem_spec = pl.BlockSpec(memory_space=pltpu.VMEM)
        dma = pltpu.SemaphoreType.DMA
        return pl.pallas_call(
            layer_kernel,
            out_shape=jax.ShapeDtypeStruct((rows, hidden), jnp.bfloat16),
            in_specs=[any_spec, vmem_spec, vmem_spec, any_spec, any_spec, any_spec],
            out_specs=vmem_spec,
            scratch_shapes=[
                pltpu.VMEM((4 * rows, hidden), BF16),
                pltpu.VMEM((4, 2 * expert_ids.shape[1], rows), F32),
                pltpu.VMEM((4 * rows, 128), F32),
                pltpu.VMEM((2, 2, n_own, hidden, ff), BF16),
                pltpu.VMEM((2, 2, n_own, hidden, ff), BF16),
                pltpu.VMEM((2, 2, n_own, ff, hidden), BF16),
                pltpu.VMEM((2, 2, n_own, 4 * rows, ff), BF16),
                pltpu.VMEM((n_cols, 4 * rows, COLS), F32),
                pltpu.VMEM((n_cols, rows, COLS), F32),
                pltpu.VMEM((n_cols, rows, COLS), F32),
                pltpu.VMEM((n_cols, rows, COLS), F32),
                dma((4,)), dma((9,)), dma((9,)),
                dma((n_own, 3)), dma((n_own, 3)),
                dma((n_z,)), dma((n_z,)), dma((n_z,)), dma((n_z,)),
                dma((n_z,)), dma((n_z,)), dma((n_z,)), dma((n_z,)),
                dma((3, n_cols, PIECES)), dma((3, n_cols, PIECES)),
            ],
            compiler_params=pltpu.CompilerParams(
                collective_id=0, has_side_effects=True, vmem_limit_bytes=67_043_328
            ),
        )(tokens, expert_ids.T, gates.T, w_gate, w_up, w_down)

    return jax.shard_map(local_layer, mesh=mesh, in_specs=(row_spec, row_spec, row_spec, P("ep", None, "tp"), P("ep", None, "tp"), P("ep", "tp", None)), out_specs=row_spec, check_vma=False)
```

```python
import functools

import jax
import jax.numpy as jnp
from jax import lax
from jax.experimental import pallas as pl
from jax.experimental.pallas import tpu as pltpu
from jax.sharding import PartitionSpec as P

MESH = pl.DeviceIdType.MESH
F32 = jnp.float32
BF16 = jnp.bfloat16

PIECES = 4
COLS = 256


def layer_kernel(
    tok_h, ids_ref, gates_ref, wg_h, wu_h, wd_h, out_ref,
    tok, raw, gm, wg, wu, wd, hid, acc, got_a, got_b, got_c,
    loc_sem, tok_ss, tok_rs, own_ss, own_rs, z_ss, z_rs, x_ss, x_rs, cz_ss, cz_rs, cx_ss, cx_rs, out_ss, out_rs,
):
    n_own, hidden, ff = wg_h.shape
    half = n_own // 2
    rows = tok_h.shape[0]
    part = rows // 2
    n_cols = hidden // COLS
    chunk = rows // PIECES
    top_k = ids_ref.shape[0]
    x = lax.axis_index("dp")
    z = lax.axis_index("tp")
    ep = lax.axis_index("ep")
    core = lax.rem(ep, 2)
    to_x = {"dp": 1 - x}
    to_y = {"ep": lax.rem(ep + 2, 4)}
    to_c = {"ep": ep + 1 - 2 * core}
    to_z = {"tp": z + 1 - 2 * lax.rem(z, 2)}
    to_zz = {"tp": lax.rem(z + 2, 4)}
    row_d, row_c, row_b, row_a = 0, rows, 2 * rows, 3 * rows

    def rcopy(src, dst, ss, rs, dev):
        return pltpu.make_async_remote_copy(
            src_ref=src, dst_ref=dst, send_sem=ss, recv_sem=rs, device_id=dev, device_id_type=MESH
        )

    bufs = (wg, wu, wd)
    hbm = (wg_h, wu_h, wd_h)

    loc = [pltpu.make_async_copy(tok_h, tok.at[pl.ds(row_d, rows)], loc_sem.at[0])]
    loc += [pltpu.make_async_copy(hbm[a], bufs[a].at[0, 0], loc_sem.at[1 + a]) for a in range(3)]
    for cp in loc:
        cp.start()
    raw[0, pl.ds(0, top_k)] = ids_ref[...].astype(F32)
    raw[0, pl.ds(top_k, top_k)] = gates_ref[...]

    barrier = pltpu.get_barrier_semaphore()
    for dev in (to_x, to_y, to_c, to_z, to_zz):
        pl.semaphore_signal(barrier, inc=1, device_id=dev, device_id_type=MESH)
    with jax.named_scope("entry"):
        pl.semaphore_wait(barrier, 5)

    def side(base, p):
        return pl.ds(base + p * part, part)

    tok_y = [rcopy(tok_h.at[side(0, p)], tok.at[side(row_c, p)], tok_ss.at[8 * p], tok_rs.at[8 * p], to_y)
             for p in range(2)]
    gat_y = rcopy(raw.at[0], raw.at[1], tok_ss.at[1], tok_rs.at[1], to_y)
    gat_z = rcopy(raw.at[0], raw.at[2], tok_ss.at[2], tok_rs.at[2], to_zz)
    gat_f = rcopy(raw.at[2], raw.at[3], tok_ss.at[3], tok_rs.at[3], to_y)
    tok_z = [rcopy(tok_h.at[side(0, p)], tok.at[side(row_b, p)], tok_ss.at[4 + p], tok_rs.at[4 + p], to_zz)
             for p in range(2)]
    tok_f = [rcopy(tok.at[side(row_b, p)], tok.at[side(row_a, p)], tok_ss.at[6 + p], tok_rs.at[6 + p], to_y)
             for p in range(2)]

    def own_c(i, a):
        return rcopy(hbm[a].at[i], bufs[a].at[0, 1, i], own_ss.at[i, a], own_rs.at[i, a], to_c)

    n_in = 2 * half
    n_z = n_in + n_cols

    def at_slot(share, n, lo):
        if n < n_in:
            return bufs[n % 2].at[1, share, lo + n // 2]
        return wd.at[1, share, pl.ds(lo, half), :, pl.ds((n - n_in) * COLS, COLS)]

    def over_z(n):
        if n < n_in:
            src = hbm[n % 2].at[x * half + n // 2]
        else:
            src = wd_h.at[pl.ds(x * half, half), :, pl.ds((n - n_in) * COLS, COLS)]
        return rcopy(src, at_slot(0, n, 0), z_ss.at[n], z_rs.at[n], to_z)

    def over_x(n):
        return rcopy(at_slot(0, n, 0), at_slot(0, n, half), x_ss.at[n], x_rs.at[n], to_x)

    def over_cz(n):
        return rcopy(at_slot(0, n, 0), at_slot(1, n, 0), cz_ss.at[n], cz_rs.at[n], to_c)

    def over_cx(n):
        return rcopy(at_slot(0, n, half), at_slot(1, n, half), cx_ss.at[n], cx_rs.at[n], to_c)

    inner_layer = lax.rem(z * (3 - z), 3) // 2
    tok_z[0].start()
    tok_y[0].start()
    gat_z.start()
    gat_y.start()
    tok_y[1].start()

    @pl.when(inner_layer == 0)
    def _():
        tok_z[1].start()

    for a in range(3):
        own_c(0, a).start()
    for n in range(n_z):
        over_z(n).start()
    for i in range(1, n_own):
        for a in range(3):
            own_c(i, a).start()

    base = (ep * n_own, (ep + 1 - 2 * core) * n_own)

    def gates_of(b):
        lane = lax.broadcasted_iota(jnp.int32, (2 * n_own, rows), 0)
        second_core = lane >= n_own
        t = jnp.where(second_core, lane - n_own, lane) + x * half
        t = jnp.where(t >= n_own, t - n_own, t)
        name = (t + jnp.where(second_core, base[1], base[0])).astype(F32)
        mine_of = jnp.zeros(name.shape, F32)
        for j in range(top_k):
            mine_of += jnp.where(name == raw[b, j : j + 1], raw[b, top_k + j : top_k + j + 1], 0.0)
        full = jnp.concatenate([mine_of, jnp.zeros((128 - 2 * n_own, rows), F32)], axis=0)
        gm[pl.ds(b * rows, rows)] = full.T

    with jax.named_scope("loc"):
        for cp in loc:
            cp.wait()
    gates_of(0)

    def slot(t):
        return (t % 2) * half + t // 2

    def inner(r, m, s, i):
        at = pl.ds(pl.multiple_of(r, m), m)
        xb = tok[at]
        for c in range(2):
            w_in = jnp.concatenate([wg[s, c, i], wu[s, c, i]], axis=1)
            both = jnp.dot(xb, w_in, preferred_element_type=F32)
            hid[s, c, i, at] = (jax.nn.silu(both[:, :ff]) * both[:, ff:]).astype(BF16)

    def first(r, m):
        def go(i, carry):
            inner(r, m, 0, i)
            return carry

        lax.fori_loop(0, n_own, go, 0)

    def second(r, m, lo, hi):
        def go(t, carry):
            inner(r, m, 1, slot(t))
            return carry

        lax.fori_loop(lo, hi, go, 0)

    def second_blocks(t, lo, hi):
        def go(b, carry):
            inner(b * rows, rows, 1, slot(t))
            return carry

        lax.fori_loop(lo, hi, go, 0)

    def down(r, k):
        at = pl.ds(r, rows)
        sl = pl.ds(pl.multiple_of(k * COLS, COLS), COLS)
        for q in range(n_own):
            i = lax.rem(x * half + q, n_own)
            total = None if q == 0 else acc[k, at]
            for c in range(2):
                h = jnp.concatenate([hid[0, c, i, at], hid[1, c, q, at]], axis=1)
                w_out = jnp.concatenate([wd[0, c, i, :, sl], wd[1, c, q, :, sl]], axis=0)
                lane = c * n_own + q
                term = gm[at, lane : lane + 1] * jnp.dot(h, w_out, preferred_element_type=F32)
                total = term if total is None else total + term
            acc[k, at] = total

    def pass_z(n):
        with jax.named_scope(f"ev_z{n}"):
            over_z(n).wait_recv()
        over_x(n).start()
        over_cz(n).start()

    def pass_x(n):
        with jax.named_scope(f"ev_x{n}"):
            over_x(n).wait_recv()
        over_cx(n).start()

    def ready(t):
        with jax.named_scope(f"ev_q{t}"):
            for n in (t - t % 2, t - t % 2 + 1):
                (over_cx(n) if t % 2 else over_cz(n)).wait_recv()

    def rows_of(j):
        return pl.ds(j * chunk, chunk)

    def out_copy(which, r, got, dev):
        def make(k, j):
            return rcopy(acc.at[k, pl.ds(r + j * chunk, chunk)], got.at[k, rows_of(j)],
                         out_ss.at[which, k, j], out_rs.at[which, k, j], dev)

        return make

    send_a = out_copy(0, row_a, got_a, to_y)
    send_b = out_copy(1, row_b, got_b, to_zz)
    send_c = out_copy(2, row_c, got_c, to_y)

    def add_a(k, j):
        with jax.named_scope(f"late_a{k}{j}"):
            send_a(k, j).wait_recv()
        at = pl.ds(row_b + j * chunk, chunk)
        acc[k, at] = acc[k, at] + got_a[k, rows_of(j)]
        send_b(k, j).start()

    def give(k, j):
        with jax.named_scope(f"late_c{k}{j}"):
            send_c(k, j).wait_recv()
        with jax.named_scope(f"late_b{k}{j}"):
            send_b(k, j).wait_recv()
        total = acc[k, rows_of(j)] + got_c[k, rows_of(j)] + got_b[k, rows_of(j)]
        out_ref[rows_of(j), pl.ds(k * COLS, COLS)] = total.astype(out_ref.dtype)

    def mine(i, carry):
        with jax.named_scope("ev_own"):
            for a in range(3):
                own_c(i, a).wait_recv()
        inner(row_d, rows, 0, i)
        return carry

    lax.fori_loop(0, n_own, mine, 0)

    def near_tokens(p):
        with jax.named_scope(f"ev_tok_c{p}"):
            tok_y[p].wait_recv()
            if p == 0:
                gat_y.wait_recv()
        if p == 0:
            gates_of(1)
        first(row_c + p * part, part)

    def b_tokens(p):
        with jax.named_scope(f"ev_tok_b{p}"):
            tok_z[p].wait_recv()
            if p == 0:
                gat_z.wait_recv()
        tok_f[p].start()
        if p == 0:
            gat_f.start()
            gates_of(2)

    def a_tokens(p):
        with jax.named_scope(f"ev_tok_a{p}"):
            tok_f[p].wait_recv()
            if p == 0:
                gat_f.wait_recv()
        if p == 0:
            gates_of(3)
        first(row_a + p * part, part)

    def middle():
        tok_z[1].start()
        near_tokens(0)
        near_tokens(1)
        b_tokens(0)
        pass_z(0)
        first(row_b, part)
        pass_z(1)
        ready(0)
        second_blocks(0, 0, 2)
        second(row_b, part, 0, 1)
        pass_z(2)
        a_tokens(0)
        pass_x(0)
        pass_x(1)
        b_tokens(1)
        pass_z(3)
        first(row_b + part, part)
        ready(1)
        second_blocks(1, 0, 2)
        second(row_b, part, 1, 2)
        second(row_b + part, part, 0, 2)
        pass_z(4)
        ready(2)
        second_blocks(2, 0, 3)
        pass_x(2)
        pass_x(3)
        second(row_a, part, 0, 3)
        pass_z(5)
        a_tokens(1)
        second(row_a + part, part, 0, 3)
        ready(3)
        second_blocks(3, 0, 2)
        pass_z(6)
        second_blocks(3, 2, 4)
        pass_x(4)
        pass_x(5)
        ready(4)
        second_blocks(4, 0, 4)
        pass_z(7)
        ready(5)
        second_blocks(5, 0, 4)
        ready(6)
        second_blocks(6, 0, 4)
        pass_z(8)
        pass_x(6)
        pass_x(7)
        ready(7)
        second_blocks(7, 0, 4)
        pass_z(9)

    def end():
        pass_z(0)
        near_tokens(0)
        pass_z(1)
        near_tokens(1)
        pass_z(2)
        pass_x(0)
        pass_x(1)
        ready(0)
        second_blocks(0, 0, 2)
        ready(1)
        second_blocks(1, 0, 2)
        pass_z(3)
        ready(2)
        second_blocks(2, 0, 2)
        b_tokens(0)
        first(row_b, part)
        second(row_b, part, 0, 3)
        pass_z(4)
        pass_x(2)
        pass_x(3)
        ready(3)
        second_blocks(3, 0, 2)
        second(row_b, part, 3, 4)
        pass_z(5)
        a_tokens(0)
        second(row_a, part, 0, 4)
        b_tokens(1)
        pass_z(6)
        pass_x(4)
        pass_x(5)
        first(row_b + part, part)
        second(row_b + part, part, 0, 4)
        ready(4)
        second_blocks(4, 0, 3)
        second(row_a, part, 4, 5)
        pass_z(7)
        ready(5)
        second_blocks(5, 0, 3)
        second(row_a, part, 5, 6)
        a_tokens(1)
        pass_z(8)
        pass_x(6)
        pass_x(7)
        second(row_a + part, part, 0, 6)
        ready(6)
        second_blocks(6, 0, 4)
        pass_z(9)
        ready(7)
        second_blocks(7, 0, 4)

    pl.when(inner_layer == 1)(middle)
    pl.when(inner_layer == 0)(end)

    def column(k, carry):
        for m in range(n_cols):
            @pl.when(k == m)
            def _(m=m):
                n = n_in + m
                pass_x(n)
                with jax.named_scope(f"ev_w{m}"):
                    over_cz(n).wait_recv()
                    over_cx(n).wait_recv()

        down(row_a, k)
        with jax.named_scope("out_a"):
            for j in range(PIECES):
                send_a(k, j).start()

        @pl.when(k == 0)
        def _():
            pass_z(n_in + 2)

        @pl.when(k == 1)
        def _():
            add_a(0, 1)

        down(row_b, k)

        @pl.when(k == 0)
        def _():
            add_a(0, 0)
            pass_z(n_in + 3)

        @pl.when(k == 1)
        def _():
            add_a(0, 2)

        @pl.when(k == 2)
        def _():
            add_a(0, 3)

        down(row_c, k)
        for j in range(PIECES):
            send_c(k, j).start()
        down(row_d, k)
        return carry

    lax.fori_loop(0, n_cols, column, 0)
    for k in range(1, n_cols):
        for j in range(PIECES):
            add_a(k, j)
            give(k - 1, j)
    for j in range(PIECES):
        give(n_cols - 1, j)

    for cp in [gat_y, gat_z, gat_f] + tok_y + tok_z + tok_f:
        cp.wait_send()
    for a in range(3):
        for i in range(n_own):
            own_c(i, a).wait_send()
    for n in range(n_z):
        for cp in (over_z(n), over_x(n), over_cz(n), over_cx(n)):
            cp.wait_send()
    for k in range(n_cols):
        for j in range(PIECES):
            for cp in (send_a(k, j), send_b(k, j), send_c(k, j)):
                cp.wait_send()


def solution(mesh):
    row_spec = P(("dp", "ep", "tp"), None)

    def local_layer(tokens, expert_ids, gates, w_gate, w_up, w_down):
        n_own = w_gate.shape[0]
        rows, hidden = tokens.shape
        ff = w_gate.shape[2]
        n_cols = hidden // COLS
        n_z = n_own + n_cols
        any_spec = pl.BlockSpec(memory_space=pl.ANY)
        vmem_spec = pl.BlockSpec(memory_space=pltpu.VMEM)
        dma = pltpu.SemaphoreType.DMA
        return pl.pallas_call(
            layer_kernel,
            out_shape=jax.ShapeDtypeStruct((rows, hidden), jnp.bfloat16),
            in_specs=[any_spec, vmem_spec, vmem_spec, any_spec, any_spec, any_spec],
            out_specs=vmem_spec,
            scratch_shapes=[
                pltpu.VMEM((4 * rows, hidden), BF16),
                pltpu.VMEM((4, 2 * expert_ids.shape[1], rows), F32),
                pltpu.VMEM((4 * rows, 128), F32),
                pltpu.VMEM((2, 2, n_own, hidden, ff), BF16),
                pltpu.VMEM((2, 2, n_own, hidden, ff), BF16),
                pltpu.VMEM((2, 2, n_own, ff, hidden), BF16),
                pltpu.VMEM((2, 2, n_own, 4 * rows, ff), BF16),
                pltpu.VMEM((n_cols, 4 * rows, COLS), F32),
                pltpu.VMEM((n_cols, rows, COLS), F32),
                pltpu.VMEM((n_cols, rows, COLS), F32),
                pltpu.VMEM((n_cols, rows, COLS), F32),
                dma((4,)), dma((9,)), dma((9,)),
                dma((n_own, 3)), dma((n_own, 3)),
                dma((n_z,)), dma((n_z,)), dma((n_z,)), dma((n_z,)),
                dma((n_z,)), dma((n_z,)), dma((n_z,)), dma((n_z,)),
                dma((3, n_cols, PIECES)), dma((3, n_cols, PIECES)),
            ],
            compiler_params=pltpu.CompilerParams(
                collective_id=0, has_side_effects=True, vmem_limit_bytes=67_043_328
            ),
        )(tokens, expert_ids.T, gates.T, w_gate, w_up, w_down)

    return jax.shard_map(local_layer, mesh=mesh, in_specs=(row_spec, row_spec, row_spec, P("ep", None, "tp"), P("ep", None, "tp"), P("ep", "tp", None)), out_specs=row_spec, check_vma=False)
```

```python
import functools

import jax
import jax.numpy as jnp
from jax import lax
from jax.experimental import pallas as pl
from jax.experimental.pallas import tpu as pltpu
from jax.sharding import PartitionSpec as P

MESH = pl.DeviceIdType.MESH
F32 = jnp.float32
BF16 = jnp.bfloat16

PIECES = 4
COLS = 256


def layer_kernel(
    tok_h, ids_ref, gates_ref, wg_h, wu_h, wd_h, out_ref,
    tok, raw, gm, wg, wu, wd, hid, acc, got_a, got_b, got_c,
    loc_sem, tok_ss, tok_rs, own_ss, own_rs, z_ss, z_rs, x_ss, x_rs, cz_ss, cz_rs, cx_ss, cx_rs, out_ss, out_rs,
):
    n_own, hidden, ff = wg_h.shape
    half = n_own // 2
    rows = tok_h.shape[0]
    part = rows // 2
    n_cols = hidden // COLS
    chunk = rows // PIECES
    top_k = ids_ref.shape[0]
    x = lax.axis_index("dp")
    z = lax.axis_index("tp")
    ep = lax.axis_index("ep")
    core = lax.rem(ep, 2)
    to_x = {"dp": 1 - x}
    to_y = {"ep": lax.rem(ep + 2, 4)}
    to_c = {"ep": ep + 1 - 2 * core}
    to_z = {"tp": z + 1 - 2 * lax.rem(z, 2)}
    to_zz = {"tp": lax.rem(z + 2, 4)}
    row_d, row_c, row_b, row_a = 0, rows, 2 * rows, 3 * rows

    def rcopy(src, dst, ss, rs, dev):
        return pltpu.make_async_remote_copy(
            src_ref=src, dst_ref=dst, send_sem=ss, recv_sem=rs, device_id=dev, device_id_type=MESH
        )

    bufs = (wg, wu, wd)
    hbm = (wg_h, wu_h, wd_h)

    loc = [pltpu.make_async_copy(tok_h, tok.at[pl.ds(row_d, rows)], loc_sem.at[0])]
    loc += [pltpu.make_async_copy(hbm[a], bufs[a].at[0, 0], loc_sem.at[1 + a]) for a in range(3)]
    for cp in loc:
        cp.start()
    raw[0, pl.ds(0, top_k)] = ids_ref[...].astype(F32)
    raw[0, pl.ds(top_k, top_k)] = gates_ref[...]

    barrier = pltpu.get_barrier_semaphore()
    for dev in (to_x, to_y, to_c, to_z, to_zz):
        pl.semaphore_signal(barrier, inc=1, device_id=dev, device_id_type=MESH)
    with jax.named_scope("entry"):
        pl.semaphore_wait(barrier, 5)

    def side(base, p):
        return pl.ds(base + p * part, part)

    tok_y = [rcopy(tok_h.at[side(0, p)], tok.at[side(row_c, p)], tok_ss.at[8 * p], tok_rs.at[8 * p], to_y)
             for p in range(2)]
    gat_y = rcopy(raw.at[0], raw.at[1], tok_ss.at[1], tok_rs.at[1], to_y)
    gat_z = rcopy(raw.at[0], raw.at[2], tok_ss.at[2], tok_rs.at[2], to_zz)
    gat_f = rcopy(raw.at[2], raw.at[3], tok_ss.at[3], tok_rs.at[3], to_y)
    tok_z = [rcopy(tok_h.at[side(0, p)], tok.at[side(row_b, p)], tok_ss.at[4 + p], tok_rs.at[4 + p], to_zz)
             for p in range(2)]
    tok_f = [rcopy(tok.at[side(row_b, p)], tok.at[side(row_a, p)], tok_ss.at[6 + p], tok_rs.at[6 + p], to_y)
             for p in range(2)]

    def own_c(i, a):
        return rcopy(hbm[a].at[i], bufs[a].at[0, 1, i], own_ss.at[i, a], own_rs.at[i, a], to_c)

    n_in = 2 * half
    n_z = n_in + n_cols

    def at_slot(share, n, lo):
        if n < n_in:
            return bufs[n % 2].at[1, share, lo + n // 2]
        return wd.at[1, share, pl.ds(lo, half), :, pl.ds((n - n_in) * COLS, COLS)]

    def over_z(n):
        if n < n_in:
            src = hbm[n % 2].at[x * half + n // 2]
        else:
            src = wd_h.at[pl.ds(x * half, half), :, pl.ds((n - n_in) * COLS, COLS)]
        return rcopy(src, at_slot(0, n, 0), z_ss.at[n], z_rs.at[n], to_z)

    def over_x(n):
        return rcopy(at_slot(0, n, 0), at_slot(0, n, half), x_ss.at[n], x_rs.at[n], to_x)

    def over_cz(n):
        return rcopy(at_slot(0, n, 0), at_slot(1, n, 0), cz_ss.at[n], cz_rs.at[n], to_c)

    def over_cx(n):
        return rcopy(at_slot(0, n, half), at_slot(1, n, half), cx_ss.at[n], cx_rs.at[n], to_c)

    inner_layer = lax.rem(z * (3 - z), 3) // 2
    tok_z[0].start()
    tok_y[0].start()
    gat_z.start()
    gat_y.start()
    tok_y[1].start()

    @pl.when(inner_layer == 0)
    def _():
        tok_z[1].start()

    for a in range(3):
        own_c(0, a).start()
    for n in range(n_z):
        over_z(n).start()
    for i in range(1, n_own):
        for a in range(3):
            own_c(i, a).start()

    base = (ep * n_own, (ep + 1 - 2 * core) * n_own)

    def gates_of(b):
        lane = lax.broadcasted_iota(jnp.int32, (2 * n_own, rows), 0)
        second_core = lane >= n_own
        t = jnp.where(second_core, lane - n_own, lane) + x * half
        t = jnp.where(t >= n_own, t - n_own, t)
        name = (t + jnp.where(second_core, base[1], base[0])).astype(F32)
        mine_of = jnp.zeros(name.shape, F32)
        for j in range(top_k):
            mine_of += jnp.where(name == raw[b, j : j + 1], raw[b, top_k + j : top_k + j + 1], 0.0)
        full = jnp.concatenate([mine_of, jnp.zeros((128 - 2 * n_own, rows), F32)], axis=0)
        gm[pl.ds(b * rows, rows)] = full.T

    with jax.named_scope("loc"):
        for cp in loc:
            cp.wait()
    gates_of(0)

    def slot(t):
        return (t % 2) * half + t // 2

    def inner(r, m, s, i):
        at = pl.ds(pl.multiple_of(r, m), m)
        xb = tok[at]
        for c in range(2):
            w_in = jnp.concatenate([wg[s, c, i], wu[s, c, i]], axis=1)
            both = jnp.dot(xb, w_in, preferred_element_type=F32)
            hid[s, c, i, at] = (jax.nn.silu(both[:, :ff]) * both[:, ff:]).astype(BF16)

    def first(r, m):
        def go(i, carry):
            inner(r, m, 0, i)
            return carry

        lax.fori_loop(0, n_own, go, 0)

    def second(r, m, lo, hi):
        def go(t, carry):
            inner(r, m, 1, slot(t))
            return carry

        lax.fori_loop(lo, hi, go, 0)

    def second_blocks(t, lo, hi):
        def go(b, carry):
            inner(b * rows, rows, 1, slot(t))
            return carry

        lax.fori_loop(lo, hi, go, 0)

    def down(r, k):
        at = pl.ds(r, rows)
        sl = pl.ds(pl.multiple_of(k * COLS, COLS), COLS)
        for q in range(n_own):
            i = lax.rem(x * half + q, n_own)
            total = None if q == 0 else acc[k, at]
            for c in range(2):
                h = jnp.concatenate([hid[0, c, i, at], hid[1, c, q, at]], axis=1)
                w_out = jnp.concatenate([wd[0, c, i, :, sl], wd[1, c, q, :, sl]], axis=0)
                lane = c * n_own + q
                term = gm[at, lane : lane + 1] * jnp.dot(h, w_out, preferred_element_type=F32)
                total = term if total is None else total + term
            acc[k, at] = total

    def pass_z(n):
        with jax.named_scope(f"ev_z{n}"):
            over_z(n).wait_recv()
        over_x(n).start()
        over_cz(n).start()

    def pass_x(n):
        with jax.named_scope(f"ev_x{n}"):
            over_x(n).wait_recv()
        over_cx(n).start()

    def ready(t):
        with jax.named_scope(f"ev_q{t}"):
            for n in (t - t % 2, t - t % 2 + 1):
                (over_cx(n) if t % 2 else over_cz(n)).wait_recv()

    def rows_of(j):
        return pl.ds(j * chunk, chunk)

    def out_copy(which, r, got, dev):
        def make(k, j):
            return rcopy(acc.at[k, pl.ds(r + j * chunk, chunk)], got.at[k, rows_of(j)],
                         out_ss.at[which, k, j], out_rs.at[which, k, j], dev)

        return make

    send_a = out_copy(0, row_a, got_a, to_y)
    send_b = out_copy(1, row_b, got_b, to_zz)
    send_c = out_copy(2, row_c, got_c, to_y)

    def add_a(k, j):
        with jax.named_scope(f"late_a{k}{j}"):
            send_a(k, j).wait_recv()
        at = pl.ds(row_b + j * chunk, chunk)
        acc[k, at] = acc[k, at] + got_a[k, rows_of(j)]
        send_b(k, j).start()

    def give(k, j):
        with jax.named_scope(f"late_c{k}{j}"):
            send_c(k, j).wait_recv()
        with jax.named_scope(f"late_b{k}{j}"):
            send_b(k, j).wait_recv()
        total = acc[k, rows_of(j)] + got_c[k, rows_of(j)] + got_b[k, rows_of(j)]
        out_ref[rows_of(j), pl.ds(k * COLS, COLS)] = total.astype(out_ref.dtype)

    def mine(i, carry):
        with jax.named_scope("ev_own"):
            for a in range(3):
                own_c(i, a).wait_recv()
        inner(row_d, rows, 0, i)
        return carry

    lax.fori_loop(0, n_own, mine, 0)

    def near_tokens(p):
        with jax.named_scope(f"ev_tok_c{p}"):
            tok_y[p].wait_recv()
            if p == 0:
                gat_y.wait_recv()
        if p == 0:
            gates_of(1)
        first(row_c + p * part, part)

    def b_tokens(p):
        with jax.named_scope(f"ev_tok_b{p}"):
            tok_z[p].wait_recv()
            if p == 0:
                gat_z.wait_recv()
        tok_f[p].start()
        if p == 0:
            gat_f.start()
            gates_of(2)

    def a_tokens(p):
        with jax.named_scope(f"ev_tok_a{p}"):
            tok_f[p].wait_recv()
            if p == 0:
                gat_f.wait_recv()
        if p == 0:
            gates_of(3)
        first(row_a + p * part, part)

    def middle():
        tok_z[1].start()
        near_tokens(0)
        near_tokens(1)
        b_tokens(0)
        pass_z(0)
        first(row_b, part)
        pass_z(1)
        ready(0)
        second_blocks(0, 0, 2)
        second(row_b, part, 0, 1)
        pass_z(2)
        a_tokens(0)
        pass_x(0)
        pass_x(1)
        b_tokens(1)
        pass_z(3)
        first(row_b + part, part)
        ready(1)
        second_blocks(1, 0, 2)
        second(row_b, part, 1, 2)
        second(row_b + part, part, 0, 2)
        pass_z(4)
        ready(2)
        second_blocks(2, 0, 3)
        pass_x(2)
        pass_x(3)
        second(row_a, part, 0, 3)
        pass_z(5)
        a_tokens(1)
        second(row_a + part, part, 0, 3)
        ready(3)
        second_blocks(3, 0, 2)
        pass_z(6)
        second_blocks(3, 2, 4)
        pass_x(4)
        pass_x(5)
        ready(4)
        second_blocks(4, 0, 4)
        pass_z(7)
        ready(5)
        second_blocks(5, 0, 4)
        ready(6)
        second_blocks(6, 0, 4)
        pass_z(8)
        pass_x(6)
        pass_x(7)
        ready(7)
        second_blocks(7, 0, 4)
        pass_z(9)

    def end():
        pass_z(0)
        near_tokens(0)
        pass_z(1)
        near_tokens(1)
        pass_z(2)
        pass_x(0)
        pass_x(1)
        ready(0)
        second_blocks(0, 0, 2)
        ready(1)
        second_blocks(1, 0, 2)
        b_tokens(0)
        first(row_b, part)
        second(row_b, part, 0, 2)
        b_tokens(1)
        pass_z(3)
        first(row_b + part, part)
        second(row_b + part, part, 0, 2)
        pass_z(4)
        a_tokens(0)
        second(row_a, part, 0, 2)
        ready(2)
        second_blocks(2, 0, 3)
        second(row_a, part, 2, 3)
        pass_x(2)
        pass_x(3)
        pass_z(5)
        ready(3)
        second_blocks(3, 0, 3)
        second(row_a, part, 3, 4)
        a_tokens(1)
        pass_z(6)
        second(row_a + part, part, 0, 4)
        pass_x(4)
        pass_x(5)
        ready(4)
        second_blocks(4, 0, 4)
        pass_z(7)
        ready(5)
        second_blocks(5, 0, 4)
        ready(6)
        second_blocks(6, 0, 4)
        pass_z(8)
        pass_x(6)
        pass_x(7)
        ready(7)
        second_blocks(7, 0, 4)
        pass_z(9)

    pl.when(inner_layer == 1)(middle)
    pl.when(inner_layer == 0)(end)

    def column(k, carry):
        for m in range(n_cols):
            @pl.when(k == m)
            def _(m=m):
                n = n_in + m
                pass_x(n)
                with jax.named_scope(f"ev_w{m}"):
                    over_cz(n).wait_recv()
                    over_cx(n).wait_recv()

        down(row_a, k)
        with jax.named_scope("out_a"):
            for j in range(PIECES):
                send_a(k, j).start()

        @pl.when(k == 0)
        def _():
            pass_z(n_in + 2)

        @pl.when(k == 1)
        def _():
            add_a(0, 1)

        down(row_b, k)

        @pl.when(k == 0)
        def _():
            add_a(0, 0)
            pass_z(n_in + 3)

        @pl.when(k == 1)
        def _():
            add_a(0, 2)

        @pl.when(k == 2)
        def _():
            add_a(0, 3)

        down(row_c, k)
        for now, blocks in ((0, (0,)), (2, (1,)), (3, (2, 3))):
            @pl.when(k == now)
            def _(blocks=blocks):
                for m in blocks:
                    for j in range(PIECES):
                        send_c(m, j).start()

        down(row_d, k)
        return carry

    lax.fori_loop(0, n_cols, column, 0)
    for add_k, give_k in ((1, 0), (2, None), (3, 1), (None, 2), (None, 3)):
        for j in range(PIECES):
            if give_k is not None:
                give(give_k, j)
            if add_k is not None:
                add_a(add_k, j)

    for cp in [gat_y, gat_z, gat_f] + tok_y + tok_z + tok_f:
        cp.wait_send()
    for a in range(3):
        for i in range(n_own):
            own_c(i, a).wait_send()
    for n in range(n_z):
        for cp in (over_z(n), over_x(n), over_cz(n), over_cx(n)):
            cp.wait_send()
    for k in range(n_cols):
        for j in range(PIECES):
            for cp in (send_a(k, j), send_b(k, j), send_c(k, j)):
                cp.wait_send()


def solution(mesh):
    row_spec = P(("dp", "ep", "tp"), None)

    def local_layer(tokens, expert_ids, gates, w_gate, w_up, w_down):
        n_own = w_gate.shape[0]
        rows, hidden = tokens.shape
        ff = w_gate.shape[2]
        n_cols = hidden // COLS
        n_z = n_own + n_cols
        any_spec = pl.BlockSpec(memory_space=pl.ANY)
        vmem_spec = pl.BlockSpec(memory_space=pltpu.VMEM)
        dma = pltpu.SemaphoreType.DMA
        return pl.pallas_call(
            layer_kernel,
            out_shape=jax.ShapeDtypeStruct((rows, hidden), jnp.bfloat16),
            in_specs=[any_spec, vmem_spec, vmem_spec, any_spec, any_spec, any_spec],
            out_specs=vmem_spec,
            scratch_shapes=[
                pltpu.VMEM((4 * rows, hidden), BF16),
                pltpu.VMEM((4, 2 * expert_ids.shape[1], rows), F32),
                pltpu.VMEM((4 * rows, 128), F32),
                pltpu.VMEM((2, 2, n_own, hidden, ff), BF16),
                pltpu.VMEM((2, 2, n_own, hidden, ff), BF16),
                pltpu.VMEM((2, 2, n_own, ff, hidden), BF16),
                pltpu.VMEM((2, 2, n_own, 4 * rows, ff), BF16),
                pltpu.VMEM((n_cols, 4 * rows, COLS), F32),
                pltpu.VMEM((n_cols, rows, COLS), F32),
                pltpu.VMEM((n_cols, rows, COLS), F32),
                pltpu.VMEM((n_cols, rows, COLS), F32),
                dma((4,)), dma((9,)), dma((9,)),
                dma((n_own, 3)), dma((n_own, 3)),
                dma((n_z,)), dma((n_z,)), dma((n_z,)), dma((n_z,)),
                dma((n_z,)), dma((n_z,)), dma((n_z,)), dma((n_z,)),
                dma((3, n_cols, PIECES)), dma((3, n_cols, PIECES)),
            ],
            compiler_params=pltpu.CompilerParams(
                collective_id=0, has_side_effects=True, vmem_limit_bytes=67_043_328
            ),
        )(tokens, expert_ids.T, gates.T, w_gate, w_up, w_down)

    return jax.shard_map(local_layer, mesh=mesh, in_specs=(row_spec, row_spec, row_spec, P("ep", None, "tp"), P("ep", None, "tp"), P("ep", "tp", None)), out_specs=row_spec, check_vma=False)
```

```python
import functools

import jax
import jax.numpy as jnp
from jax import lax
from jax.experimental import pallas as pl
from jax.experimental.pallas import tpu as pltpu
from jax.sharding import PartitionSpec as P

MESH = pl.DeviceIdType.MESH
F32 = jnp.float32
BF16 = jnp.bfloat16

PIECES = 4
COLS = 256


def layer_kernel(
    tok_h, ids_ref, gates_ref, wg_h, wu_h, wd_h, out_ref,
    tok, raw, gm, wg, wu, wd, hid, acc, got_a, got_b, got_c,
    loc_sem, tok_ss, tok_rs, own_ss, own_rs, z_ss, z_rs, x_ss, x_rs, cz_ss, cz_rs, cx_ss, cx_rs, out_ss, out_rs,
):
    n_own, hidden, ff = wg_h.shape
    half = n_own // 2
    rows = tok_h.shape[0]
    part = rows // 2
    n_cols = hidden // COLS
    chunk = rows // PIECES
    top_k = ids_ref.shape[0]
    x = lax.axis_index("dp")
    z = lax.axis_index("tp")
    ep = lax.axis_index("ep")
    core = lax.rem(ep, 2)
    to_x = {"dp": 1 - x}
    to_y = {"ep": lax.rem(ep + 2, 4)}
    to_c = {"ep": ep + 1 - 2 * core}
    to_z = {"tp": z + 1 - 2 * lax.rem(z, 2)}
    to_zz = {"tp": lax.rem(z + 2, 4)}
    row_d, row_c, row_b, row_a = 0, rows, 2 * rows, 3 * rows

    def rcopy(src, dst, ss, rs, dev):
        return pltpu.make_async_remote_copy(
            src_ref=src, dst_ref=dst, send_sem=ss, recv_sem=rs, device_id=dev, device_id_type=MESH
        )

    bufs = (wg, wu, wd)
    hbm = (wg_h, wu_h, wd_h)

    loc = [pltpu.make_async_copy(tok_h, tok.at[pl.ds(row_d, rows)], loc_sem.at[0])]
    loc += [pltpu.make_async_copy(hbm[a], bufs[a].at[0, 0], loc_sem.at[1 + a]) for a in range(3)]
    for cp in loc:
        cp.start()
    raw[0, pl.ds(0, top_k)] = ids_ref[...].astype(F32)
    raw[0, pl.ds(top_k, top_k)] = gates_ref[...]

    barrier = pltpu.get_barrier_semaphore()
    for dev in (to_x, to_y, to_c, to_z, to_zz):
        pl.semaphore_signal(barrier, inc=1, device_id=dev, device_id_type=MESH)
    with jax.named_scope("entry"):
        pl.semaphore_wait(barrier, 5)

    def side(base, p):
        return pl.ds(base + p * part, part)

    tok_y = [rcopy(tok_h.at[side(0, p)], tok.at[side(row_c, p)], tok_ss.at[8 * p], tok_rs.at[8 * p], to_y)
             for p in range(2)]
    gat_y = rcopy(raw.at[0], raw.at[1], tok_ss.at[1], tok_rs.at[1], to_y)
    gat_z = rcopy(raw.at[0], raw.at[2], tok_ss.at[2], tok_rs.at[2], to_zz)
    gat_f = rcopy(raw.at[2], raw.at[3], tok_ss.at[3], tok_rs.at[3], to_y)
    tok_z = [rcopy(tok_h.at[side(0, p)], tok.at[side(row_b, p)], tok_ss.at[4 + p], tok_rs.at[4 + p], to_zz)
             for p in range(2)]
    tok_f = [rcopy(tok.at[side(row_b, p)], tok.at[side(row_a, p)], tok_ss.at[6 + p], tok_rs.at[6 + p], to_y)
             for p in range(2)]

    def own_c(i, a):
        return rcopy(hbm[a].at[i], bufs[a].at[0, 1, i], own_ss.at[i, a], own_rs.at[i, a], to_c)

    n_in = 2 * half
    n_z = n_in + n_cols

    def at_slot(share, n, lo):
        if n < n_in:
            return bufs[n % 2].at[1, share, lo + n // 2]
        return wd.at[1, share, pl.ds(lo, half), :, pl.ds((n - n_in) * COLS, COLS)]

    def over_z(n):
        if n < n_in:
            src = hbm[n % 2].at[x * half + n // 2]
        else:
            src = wd_h.at[pl.ds(x * half, half), :, pl.ds((n - n_in) * COLS, COLS)]
        return rcopy(src, at_slot(0, n, 0), z_ss.at[n], z_rs.at[n], to_z)

    def over_x(n):
        return rcopy(at_slot(0, n, 0), at_slot(0, n, half), x_ss.at[n], x_rs.at[n], to_x)

    def over_cz(n):
        return rcopy(at_slot(0, n, 0), at_slot(1, n, 0), cz_ss.at[n], cz_rs.at[n], to_c)

    def over_cx(n):
        return rcopy(at_slot(0, n, half), at_slot(1, n, half), cx_ss.at[n], cx_rs.at[n], to_c)

    inner_layer = lax.rem(z * (3 - z), 3) // 2
    tok_z[0].start()
    tok_y[0].start()
    gat_z.start()
    gat_y.start()
    tok_y[1].start()

    @pl.when(inner_layer == 0)
    def _():
        tok_z[1].start()

    for a in range(3):
        own_c(0, a).start()
    for n in range(n_z):
        over_z(n).start()
    for i in range(1, n_own):
        for a in range(3):
            own_c(i, a).start()

    base = (ep * n_own, (ep + 1 - 2 * core) * n_own)

    def gates_of(b):
        lane = lax.broadcasted_iota(jnp.int32, (2 * n_own, rows), 0)
        second_core = lane >= n_own
        t = jnp.where(second_core, lane - n_own, lane) + x * half
        t = jnp.where(t >= n_own, t - n_own, t)
        name = (t + jnp.where(second_core, base[1], base[0])).astype(F32)
        mine_of = jnp.zeros(name.shape, F32)
        for j in range(top_k):
            mine_of += jnp.where(name == raw[b, j : j + 1], raw[b, top_k + j : top_k + j + 1], 0.0)
        full = jnp.concatenate([mine_of, jnp.zeros((128 - 2 * n_own, rows), F32)], axis=0)
        gm[pl.ds(b * rows, rows)] = full.T

    with jax.named_scope("loc"):
        for cp in loc:
            cp.wait()
    gates_of(0)

    def slot(t):
        return (t % 2) * half + t // 2

    def inner(r, m, s, i):
        at = pl.ds(pl.multiple_of(r, m), m)
        xb = tok[at]
        for c in range(2):
            w_in = jnp.concatenate([wg[s, c, i], wu[s, c, i]], axis=1)
            both = jnp.dot(xb, w_in, preferred_element_type=F32)
            hid[s, c, i, at] = (jax.nn.silu(both[:, :ff]) * both[:, ff:]).astype(BF16)

    def first(r, m):
        def go(i, carry):
            inner(r, m, 0, i)
            return carry

        lax.fori_loop(0, n_own, go, 0)

    def second(r, m, lo, hi):
        def go(t, carry):
            inner(r, m, 1, slot(t))
            return carry

        lax.fori_loop(lo, hi, go, 0)

    def second_blocks(t, lo, hi):
        def go(b, carry):
            inner(b * rows, rows, 1, slot(t))
            return carry

        lax.fori_loop(lo, hi, go, 0)

    def down(r, k):
        at = pl.ds(r, rows)
        sl = pl.ds(pl.multiple_of(k * COLS, COLS), COLS)
        for q in range(n_own):
            i = lax.rem(x * half + q, n_own)
            total = None if q == 0 else acc[k, at]
            for c in range(2):
                h = jnp.concatenate([hid[0, c, i, at], hid[1, c, q, at]], axis=1)
                w_out = jnp.concatenate([wd[0, c, i, :, sl], wd[1, c, q, :, sl]], axis=0)
                lane = c * n_own + q
                term = gm[at, lane : lane + 1] * jnp.dot(h, w_out, preferred_element_type=F32)
                total = term if total is None else total + term
            acc[k, at] = total

    def pass_z(n):
        with jax.named_scope(f"ev_z{n}"):
            over_z(n).wait_recv()
        over_x(n).start()
        over_cz(n).start()

    def pass_x(n):
        with jax.named_scope(f"ev_x{n}"):
            over_x(n).wait_recv()
        over_cx(n).start()

    def ready(t):
        with jax.named_scope(f"ev_q{t}"):
            for n in (t - t % 2, t - t % 2 + 1):
                (over_cx(n) if t % 2 else over_cz(n)).wait_recv()

    def rows_of(j):
        return pl.ds(j * chunk, chunk)

    def out_copy(which, r, got, dev):
        def make(k, j):
            return rcopy(acc.at[k, pl.ds(r + j * chunk, chunk)], got.at[k, rows_of(j)],
                         out_ss.at[which, k, j], out_rs.at[which, k, j], dev)

        return make

    send_a = out_copy(0, row_a, got_a, to_y)
    send_b = out_copy(1, row_b, got_b, to_zz)
    send_c = out_copy(2, row_c, got_c, to_y)

    def add_a(k, j):
        with jax.named_scope(f"late_a{k}{j}"):
            send_a(k, j).wait_recv()
        at = pl.ds(row_b + j * chunk, chunk)
        acc[k, at] = acc[k, at] + got_a[k, rows_of(j)]
        send_b(k, j).start()

    def give(k, j):
        with jax.named_scope(f"late_c{k}{j}"):
            send_c(k, j).wait_recv()
        with jax.named_scope(f"late_b{k}{j}"):
            send_b(k, j).wait_recv()
        total = acc[k, rows_of(j)] + got_c[k, rows_of(j)] + got_b[k, rows_of(j)]
        out_ref[rows_of(j), pl.ds(k * COLS, COLS)] = total.astype(out_ref.dtype)

    def mine(i, carry):
        with jax.named_scope("ev_own"):
            for a in range(3):
                own_c(i, a).wait_recv()
        inner(row_d, rows, 0, i)
        return carry

    lax.fori_loop(0, n_own, mine, 0)

    def near_tokens(p):
        with jax.named_scope(f"ev_tok_c{p}"):
            tok_y[p].wait_recv()
            if p == 0:
                gat_y.wait_recv()
        if p == 0:
            gates_of(1)
        first(row_c + p * part, part)

    def b_tokens(p):
        with jax.named_scope(f"ev_tok_b{p}"):
            tok_z[p].wait_recv()
            if p == 0:
                gat_z.wait_recv()
        tok_f[p].start()
        if p == 0:
            gat_f.start()
            gates_of(2)

    def a_tokens(p):
        with jax.named_scope(f"ev_tok_a{p}"):
            tok_f[p].wait_recv()
            if p == 0:
                gat_f.wait_recv()
        if p == 0:
            gates_of(3)
        first(row_a + p * part, part)

    def middle():
        tok_z[1].start()
        near_tokens(0)
        near_tokens(1)
        b_tokens(0)
        pass_z(0)
        first(row_b, part)
        pass_z(1)
        ready(0)
        second_blocks(0, 0, 2)
        second(row_b, part, 0, 1)
        pass_z(2)
        a_tokens(0)
        pass_x(0)
        pass_x(1)
        b_tokens(1)
        pass_z(3)
        first(row_b + part, part)
        ready(1)
        second_blocks(1, 0, 2)
        second(row_b, part, 1, 2)
        second(row_b + part, part, 0, 2)
        pass_z(4)
        ready(2)
        second_blocks(2, 0, 3)
        pass_x(2)
        pass_x(3)
        second(row_a, part, 0, 3)
        pass_z(5)
        a_tokens(1)
        second(row_a + part, part, 0, 3)
        ready(3)
        second_blocks(3, 0, 2)
        pass_z(6)
        second_blocks(3, 2, 4)
        pass_x(4)
        pass_x(5)
        ready(4)
        second_blocks(4, 1, 4)
        pass_z(7)
        ready(5)
        second_blocks(5, 1, 4)
        ready(6)
        second_blocks(6, 2, 4)
        pass_z(8)
        pass_x(6)
        pass_x(7)
        ready(7)
        second_blocks(7, 2, 4)
        pass_z(9)

    def end():
        pass_z(0)
        near_tokens(0)
        pass_z(1)
        near_tokens(1)
        pass_z(2)
        pass_x(0)
        pass_x(1)
        ready(0)
        second_blocks(0, 0, 2)
        ready(1)
        second_blocks(1, 0, 2)
        b_tokens(0)
        first(row_b, part)
        second(row_b, part, 0, 2)
        b_tokens(1)
        pass_z(3)
        first(row_b + part, part)
        second(row_b + part, part, 0, 2)
        pass_z(4)
        a_tokens(0)
        second(row_a, part, 0, 2)
        ready(2)
        second_blocks(2, 1, 3)
        second(row_a, part, 2, 3)
        pass_x(2)
        pass_x(3)
        pass_z(5)
        ready(3)
        second_blocks(3, 1, 3)
        second(row_a, part, 3, 4)
        a_tokens(1)
        pass_z(6)
        second(row_a + part, part, 0, 4)
        pass_x(4)
        pass_x(5)
        ready(4)
        second_blocks(4, 1, 4)
        pass_z(7)
        ready(5)
        second_blocks(5, 1, 4)
        ready(6)
        second_blocks(6, 2, 4)
        pass_z(8)
        pass_x(6)
        pass_x(7)
        ready(7)
        second_blocks(7, 2, 4)
        pass_z(9)

    pl.when(inner_layer == 1)(middle)
    pl.when(inner_layer == 0)(end)

    def column(k, carry):
        for m in range(n_cols):
            @pl.when(k == m)
            def _(m=m):
                n = n_in + m
                pass_x(n)
                with jax.named_scope(f"ev_w{m}"):
                    over_cz(n).wait_recv()
                    over_cx(n).wait_recv()

        down(row_a, k)
        with jax.named_scope("out_a"):
            for j in range(PIECES):
                send_a(k, j).start()

        @pl.when(k == 1)
        def _():
            add_a(0, 1)

        down(row_b, k)

        @pl.when(k == 0)
        def _():
            second(row_d, rows, 2 + 2 * inner_layer, n_own)
            pass_z(n_in + 2)
            add_a(0, 0)
            second(row_c, rows, n_own - 2, n_own)

        @pl.when(k == 1)
        def _():
            add_a(0, 2)

        @pl.when(k == 2)
        def _():
            add_a(0, 3)

        down(row_c, k)
        for now, blocks in ((0, (0,)), (2, (1,)), (3, (2, 3))):
            @pl.when(k == now)
            def _(blocks=blocks):
                for m in blocks:
                    for j in range(PIECES):
                        send_c(m, j).start()

        @pl.when(k == 0)
        def _():
            pass_z(n_in + 3)

        down(row_d, k)
        return carry

    lax.fori_loop(0, n_cols, column, 0)
    for add_k, give_k in ((1, 0), (2, None), (3, 1), (None, 2), (None, 3)):
        for j in range(PIECES):
            if give_k is not None:
                give(give_k, j)
            if add_k is not None:
                add_a(add_k, j)

    for cp in [gat_y, gat_z, gat_f] + tok_y + tok_z + tok_f:
        cp.wait_send()
    for a in range(3):
        for i in range(n_own):
            own_c(i, a).wait_send()
    for n in range(n_z):
        for cp in (over_z(n), over_x(n), over_cz(n), over_cx(n)):
            cp.wait_send()
    for k in range(n_cols):
        for j in range(PIECES):
            for cp in (send_a(k, j), send_b(k, j), send_c(k, j)):
                cp.wait_send()


def solution(mesh):
    row_spec = P(("dp", "ep", "tp"), None)

    def local_layer(tokens, expert_ids, gates, w_gate, w_up, w_down):
        n_own = w_gate.shape[0]
        rows, hidden = tokens.shape
        ff = w_gate.shape[2]
        n_cols = hidden // COLS
        n_z = n_own + n_cols
        any_spec = pl.BlockSpec(memory_space=pl.ANY)
        vmem_spec = pl.BlockSpec(memory_space=pltpu.VMEM)
        dma = pltpu.SemaphoreType.DMA
        return pl.pallas_call(
            layer_kernel,
            out_shape=jax.ShapeDtypeStruct((rows, hidden), jnp.bfloat16),
            in_specs=[any_spec, vmem_spec, vmem_spec, any_spec, any_spec, any_spec],
            out_specs=vmem_spec,
            scratch_shapes=[
                pltpu.VMEM((4 * rows, hidden), BF16),
                pltpu.VMEM((4, 2 * expert_ids.shape[1], rows), F32),
                pltpu.VMEM((4 * rows, 128), F32),
                pltpu.VMEM((2, 2, n_own, hidden, ff), BF16),
                pltpu.VMEM((2, 2, n_own, hidden, ff), BF16),
                pltpu.VMEM((2, 2, n_own, ff, hidden), BF16),
                pltpu.VMEM((2, 2, n_own, 4 * rows, ff), BF16),
                pltpu.VMEM((n_cols, 4 * rows, COLS), F32),
                pltpu.VMEM((n_cols, rows, COLS), F32),
                pltpu.VMEM((n_cols, rows, COLS), F32),
                pltpu.VMEM((n_cols, rows, COLS), F32),
                dma((4,)), dma((9,)), dma((9,)),
                dma((n_own, 3)), dma((n_own, 3)),
                dma((n_z,)), dma((n_z,)), dma((n_z,)), dma((n_z,)),
                dma((n_z,)), dma((n_z,)), dma((n_z,)), dma((n_z,)),
                dma((3, n_cols, PIECES)), dma((3, n_cols, PIECES)),
            ],
            compiler_params=pltpu.CompilerParams(
                collective_id=0, has_side_effects=True, vmem_limit_bytes=67_043_328
            ),
        )(tokens, expert_ids.T, gates.T, w_gate, w_up, w_down)

    return jax.shard_map(local_layer, mesh=mesh, in_specs=(row_spec, row_spec, row_spec, P("ep", None, "tp"), P("ep", None, "tp"), P("ep", "tp", None)), out_specs=row_spec, check_vma=False)
```

```python
import functools

import jax
import jax.numpy as jnp
from jax import lax
from jax.experimental import pallas as pl
from jax.experimental.pallas import tpu as pltpu
from jax.sharding import PartitionSpec as P

MESH = pl.DeviceIdType.MESH
F32 = jnp.float32
BF16 = jnp.bfloat16

PIECES = 4
COLS = 256


def layer_kernel(
    tok_h, ids_ref, gates_ref, wg_h, wu_h, wd_h, out_ref,
    tok, raw, gm, wg, wu, wd, hid, acc, got_a, got_b, got_c,
    loc_sem, tok_ss, tok_rs, own_ss, own_rs, z_ss, z_rs, x_ss, x_rs, cz_ss, cz_rs, cx_ss, cx_rs, out_ss, out_rs,
):
    n_own, hidden, ff = wg_h.shape
    half = n_own // 2
    rows = tok_h.shape[0]
    part = rows // 2
    n_cols = hidden // COLS
    chunk = rows // PIECES
    top_k = ids_ref.shape[0]
    x = lax.axis_index("dp")
    z = lax.axis_index("tp")
    ep = lax.axis_index("ep")
    core = lax.rem(ep, 2)
    to_x = {"dp": 1 - x}
    to_y = {"ep": lax.rem(ep + 2, 4)}
    to_c = {"ep": ep + 1 - 2 * core}
    to_z = {"tp": z + 1 - 2 * lax.rem(z, 2)}
    to_zz = {"tp": lax.rem(z + 2, 4)}
    row_d, row_c, row_b, row_a = 0, rows, 2 * rows, 3 * rows

    def rcopy(src, dst, ss, rs, dev):
        return pltpu.make_async_remote_copy(
            src_ref=src, dst_ref=dst, send_sem=ss, recv_sem=rs, device_id=dev, device_id_type=MESH
        )

    bufs = (wg, wu, wd)
    hbm = (wg_h, wu_h, wd_h)

    loc = [pltpu.make_async_copy(tok_h, tok.at[pl.ds(row_d, rows)], loc_sem.at[0])]
    loc += [pltpu.make_async_copy(hbm[a], bufs[a].at[0, 0], loc_sem.at[1 + a]) for a in range(3)]
    for cp in loc:
        cp.start()
    raw[0, pl.ds(0, top_k)] = ids_ref[...].astype(F32)
    raw[0, pl.ds(top_k, top_k)] = gates_ref[...]

    barrier = pltpu.get_barrier_semaphore()
    for dev in (to_x, to_y, to_c, to_z, to_zz):
        pl.semaphore_signal(barrier, inc=1, device_id=dev, device_id_type=MESH)
    with jax.named_scope("entry"):
        pl.semaphore_wait(barrier, 5)

    def side(base, p):
        return pl.ds(base + p * part, part)

    tok_y = [rcopy(tok_h.at[side(0, p)], tok.at[side(row_c, p)], tok_ss.at[8 * p], tok_rs.at[8 * p], to_y)
             for p in range(2)]
    gat_y = rcopy(raw.at[0], raw.at[1], tok_ss.at[1], tok_rs.at[1], to_y)
    gat_z = rcopy(raw.at[0], raw.at[2], tok_ss.at[2], tok_rs.at[2], to_zz)
    gat_f = rcopy(raw.at[2], raw.at[3], tok_ss.at[3], tok_rs.at[3], to_y)
    tok_z = [rcopy(tok_h.at[side(0, p)], tok.at[side(row_b, p)], tok_ss.at[4 + p], tok_rs.at[4 + p], to_zz)
             for p in range(2)]
    tok_f = [rcopy(tok.at[side(row_b, p)], tok.at[side(row_a, p)], tok_ss.at[6 + p], tok_rs.at[6 + p], to_y)
             for p in range(2)]

    def own_c(i, a):
        return rcopy(hbm[a].at[i], bufs[a].at[0, 1, i], own_ss.at[i, a], own_rs.at[i, a], to_c)

    n_in = 2 * half
    n_z = n_in + n_cols

    def at_slot(share, n, lo):
        if n < n_in:
            return bufs[n % 2].at[1, share, lo + n // 2]
        return wd.at[1, share, pl.ds(lo, half), :, pl.ds((n - n_in) * COLS, COLS)]

    def over_z(n):
        if n < n_in:
            src = hbm[n % 2].at[x * half + n // 2]
        else:
            src = wd_h.at[pl.ds(x * half, half), :, pl.ds((n - n_in) * COLS, COLS)]
        return rcopy(src, at_slot(0, n, 0), z_ss.at[n], z_rs.at[n], to_z)

    def over_x(n):
        return rcopy(at_slot(0, n, 0), at_slot(0, n, half), x_ss.at[n], x_rs.at[n], to_x)

    def over_cz(n):
        return rcopy(at_slot(0, n, 0), at_slot(1, n, 0), cz_ss.at[n], cz_rs.at[n], to_c)

    def over_cx(n):
        return rcopy(at_slot(0, n, half), at_slot(1, n, half), cx_ss.at[n], cx_rs.at[n], to_c)

    inner_layer = lax.rem(z * (3 - z), 3) // 2
    tok_z[0].start()
    tok_y[0].start()
    gat_z.start()
    gat_y.start()
    tok_y[1].start()

    @pl.when(inner_layer == 0)
    def _():
        tok_z[1].start()

    for a in range(3):
        own_c(0, a).start()
    for n in range(n_z):
        over_z(n).start()
    for i in range(1, n_own):
        for a in range(3):
            own_c(i, a).start()

    base = (ep * n_own, (ep + 1 - 2 * core) * n_own)

    def gates_of(b):
        lane = lax.broadcasted_iota(jnp.int32, (2 * n_own, rows), 0)
        second_core = lane >= n_own
        t = jnp.where(second_core, lane - n_own, lane) + x * half
        t = jnp.where(t >= n_own, t - n_own, t)
        name = (t + jnp.where(second_core, base[1], base[0])).astype(F32)
        mine_of = jnp.zeros(name.shape, F32)
        for j in range(top_k):
            mine_of += jnp.where(name == raw[b, j : j + 1], raw[b, top_k + j : top_k + j + 1], 0.0)
        full = jnp.concatenate([mine_of, jnp.zeros((128 - 2 * n_own, rows), F32)], axis=0)
        gm[pl.ds(b * rows, rows)] = full.T

    with jax.named_scope("loc"):
        for cp in loc:
            cp.wait()
    gates_of(0)

    def slot(t):
        return (t % 2) * half + t // 2

    def inner(r, m, s, i):
        at = pl.ds(pl.multiple_of(r, m), m)
        xb = tok[at]
        for c in range(2):
            w_in = jnp.concatenate([wg[s, c, i], wu[s, c, i]], axis=1)
            both = jnp.dot(xb, w_in, preferred_element_type=F32)
            hid[s, c, i, at] = (jax.nn.silu(both[:, :ff]) * both[:, ff:]).astype(BF16)

    def first(r, m):
        def go(i, carry):
            inner(r, m, 0, i)
            return carry

        lax.fori_loop(0, n_own, go, 0)

    def second(r, m, lo, hi):
        def go(t, carry):
            inner(r, m, 1, slot(t))
            return carry

        lax.fori_loop(lo, hi, go, 0)

    def second_blocks(t, lo, hi):
        def go(b, carry):
            inner(b * rows, rows, 1, slot(t))
            return carry

        lax.fori_loop(lo, hi, go, 0)

    def down(r, k):
        at = pl.ds(r, rows)
        sl = pl.ds(pl.multiple_of(k * COLS, COLS), COLS)
        for q in range(n_own):
            i = lax.rem(x * half + q, n_own)
            total = None if q == 0 else acc[k, at]
            for c in range(2):
                h = jnp.concatenate([hid[0, c, i, at], hid[1, c, q, at]], axis=1)
                w_out = jnp.concatenate([wd[0, c, i, :, sl], wd[1, c, q, :, sl]], axis=0)
                lane = c * n_own + q
                term = gm[at, lane : lane + 1] * jnp.dot(h, w_out, preferred_element_type=F32)
                total = term if total is None else total + term
            acc[k, at] = total

    def pass_z(n):
        with jax.named_scope(f"ev_z{n}"):
            over_z(n).wait_recv()
        over_x(n).start()
        over_cz(n).start()

    def pass_x(n):
        with jax.named_scope(f"ev_x{n}"):
            over_x(n).wait_recv()
        over_cx(n).start()

    def ready(t):
        with jax.named_scope(f"ev_q{t}"):
            for n in (t - t % 2, t - t % 2 + 1):
                (over_cx(n) if t % 2 else over_cz(n)).wait_recv()

    def rows_of(j):
        return pl.ds(j * chunk, chunk)

    def out_copy(which, r, got, dev):
        def make(k, j):
            return rcopy(acc.at[k, pl.ds(r + j * chunk, chunk)], got.at[k, rows_of(j)],
                         out_ss.at[which, k, j], out_rs.at[which, k, j], dev)

        return make

    send_a = out_copy(0, row_a, got_a, to_y)
    send_b = out_copy(1, row_b, got_b, to_zz)
    send_c = out_copy(2, row_c, got_c, to_y)

    def add_a(k, j):
        with jax.named_scope(f"late_a{k}{j}"):
            send_a(k, j).wait_recv()
        at = pl.ds(row_b + j * chunk, chunk)
        acc[k, at] = acc[k, at] + got_a[k, rows_of(j)]
        send_b(k, j).start()

    def give(k, j):
        with jax.named_scope(f"late_c{k}{j}"):
            send_c(k, j).wait_recv()
        with jax.named_scope(f"late_b{k}{j}"):
            send_b(k, j).wait_recv()
        total = acc[k, rows_of(j)] + got_c[k, rows_of(j)] + got_b[k, rows_of(j)]
        out_ref[rows_of(j), pl.ds(k * COLS, COLS)] = total.astype(out_ref.dtype)

    def mine(i, carry):
        with jax.named_scope("ev_own"):
            for a in range(3):
                own_c(i, a).wait_recv()
        inner(row_d, rows, 0, i)
        return carry

    lax.fori_loop(0, n_own, mine, 0)

    def near_tokens(p):
        with jax.named_scope(f"ev_tok_c{p}"):
            tok_y[p].wait_recv()
            if p == 0:
                gat_y.wait_recv()
        if p == 0:
            gates_of(1)
        first(row_c + p * part, part)

    def b_tokens(p):
        with jax.named_scope(f"ev_tok_b{p}"):
            tok_z[p].wait_recv()
            if p == 0:
                gat_z.wait_recv()
        tok_f[p].start()
        if p == 0:
            gat_f.start()
            gates_of(2)

    def a_tokens(p):
        with jax.named_scope(f"ev_tok_a{p}"):
            tok_f[p].wait_recv()
            if p == 0:
                gat_f.wait_recv()
        if p == 0:
            gates_of(3)
        first(row_a + p * part, part)

    def middle():
        tok_z[1].start()
        near_tokens(0)
        near_tokens(1)
        b_tokens(0)
        pass_z(0)
        first(row_b, part)
        pass_z(1)
        ready(0)
        second_blocks(0, 0, 2)
        second(row_b, part, 0, 1)
        pass_z(2)
        a_tokens(0)
        pass_x(0)
        pass_x(1)
        b_tokens(1)
        pass_z(3)
        first(row_b + part, part)
        ready(1)
        second_blocks(1, 0, 2)
        second(row_b, part, 1, 2)
        second(row_b + part, part, 0, 2)
        pass_z(4)
        ready(2)
        second_blocks(2, 0, 3)
        pass_x(2)
        pass_x(3)
        second(row_a, part, 0, 3)
        pass_z(5)
        a_tokens(1)
        second(row_a + part, part, 0, 3)
        ready(3)
        second_blocks(3, 0, 2)
        pass_z(6)
        second_blocks(3, 2, 4)
        pass_x(4)
        pass_x(5)
        ready(4)
        second_blocks(4, 1, 4)
        pass_z(7)
        ready(5)
        second_blocks(5, 1, 4)
        ready(6)
        second_blocks(6, 2, 4)
        pass_z(8)
        pass_x(6)
        pass_x(7)
        ready(7)
        second_blocks(7, 2, 4)
        pass_z(9)

    def end():
        pass_z(0)
        near_tokens(0)
        pass_z(1)
        near_tokens(1)
        pass_z(2)
        pass_x(0)
        pass_x(1)
        ready(0)
        second_blocks(0, 0, 2)
        ready(1)
        second_blocks(1, 0, 2)
        b_tokens(0)
        first(row_b, part)
        second(row_b, part, 0, 2)
        b_tokens(1)
        pass_z(3)
        first(row_b + part, part)
        second(row_b + part, part, 0, 2)
        pass_z(4)
        a_tokens(0)
        second(row_a, part, 0, 2)
        ready(2)
        second_blocks(2, 1, 3)
        second(row_a, part, 2, 3)
        pass_x(2)
        pass_x(3)
        pass_z(5)
        ready(3)
        second_blocks(3, 1, 3)
        second(row_a, part, 3, 4)
        a_tokens(1)
        pass_z(6)
        second(row_a + part, part, 0, 4)
        pass_x(4)
        pass_x(5)
        ready(4)
        second_blocks(4, 1, 4)
        pass_z(7)
        ready(5)
        second_blocks(5, 1, 4)
        ready(6)
        second_blocks(6, 2, 4)
        pass_z(8)
        pass_x(6)
        pass_x(7)
        ready(7)
        second_blocks(7, 2, 4)
        pass_z(9)

    pl.when(inner_layer == 1)(middle)
    pl.when(inner_layer == 0)(end)

    def column(k, carry):
        for m in range(n_cols):
            @pl.when(k == m)
            def _(m=m):
                n = n_in + m
                if m == 0:
                    pass_x(n)
                with jax.named_scope(f"ev_w{m}"):
                    over_cz(n).wait_recv()
                    over_cx(n).wait_recv()

        down(row_a, k)
        with jax.named_scope("out_a"):
            for j in range(PIECES):
                send_a(k, j).start()

        @pl.when(k == 1)
        def _():
            add_a(0, 1)

        down(row_b, k)

        @pl.when(k == 0)
        def _():
            put_off = 2 + 2 * inner_layer
            second(row_d, rows, put_off, put_off + 3)
            add_a(0, 0)
            pass_z(n_in + 2)
            second(row_d, rows, put_off + 3, n_own)
            second(row_c, rows, n_own - 2, n_own)

        @pl.when(k == 1)
        def _():
            add_a(0, 2)

        @pl.when(k == 2)
        def _():
            add_a(0, 3)

        down(row_c, k)
        for now, blocks in ((0, (0,)), (2, (1,)), (3, (2, 3))):
            @pl.when(k == now)
            def _(blocks=blocks):
                for m in blocks:
                    for j in range(PIECES):
                        send_c(m, j).start()

        for m in range(1, n_cols):
            @pl.when(k == m - 1)
            def _(m=m):
                if m == 1:
                    pass_z(n_in + 3)
                pass_x(n_in + m)

        down(row_d, k)
        return carry

    lax.fori_loop(0, n_cols, column, 0)
    for add_k, give_k in ((1, 0), (2, None), (3, 1), (None, 2), (None, 3)):
        for j in range(PIECES):
            if give_k is not None:
                give(give_k, j)
            if add_k is not None:
                add_a(add_k, j)

    for cp in [gat_y, gat_z, gat_f] + tok_y + tok_z + tok_f:
        cp.wait_send()
    for a in range(3):
        for i in range(n_own):
            own_c(i, a).wait_send()
    for n in range(n_z):
        for cp in (over_z(n), over_x(n), over_cz(n), over_cx(n)):
            cp.wait_send()
    for k in range(n_cols):
        for j in range(PIECES):
            for cp in (send_a(k, j), send_b(k, j), send_c(k, j)):
                cp.wait_send()


def solution(mesh):
    row_spec = P(("dp", "ep", "tp"), None)

    def local_layer(tokens, expert_ids, gates, w_gate, w_up, w_down):
        n_own = w_gate.shape[0]
        rows, hidden = tokens.shape
        ff = w_gate.shape[2]
        n_cols = hidden // COLS
        n_z = n_own + n_cols
        any_spec = pl.BlockSpec(memory_space=pl.ANY)
        vmem_spec = pl.BlockSpec(memory_space=pltpu.VMEM)
        dma = pltpu.SemaphoreType.DMA
        return pl.pallas_call(
            layer_kernel,
            out_shape=jax.ShapeDtypeStruct((rows, hidden), jnp.bfloat16),
            in_specs=[any_spec, vmem_spec, vmem_spec, any_spec, any_spec, any_spec],
            out_specs=vmem_spec,
            scratch_shapes=[
                pltpu.VMEM((4 * rows, hidden), BF16),
                pltpu.VMEM((4, 2 * expert_ids.shape[1], rows), F32),
                pltpu.VMEM((4 * rows, 128), F32),
                pltpu.VMEM((2, 2, n_own, hidden, ff), BF16),
                pltpu.VMEM((2, 2, n_own, hidden, ff), BF16),
                pltpu.VMEM((2, 2, n_own, ff, hidden), BF16),
                pltpu.VMEM((2, 2, n_own, 4 * rows, ff), BF16),
                pltpu.VMEM((n_cols, 4 * rows, COLS), F32),
                pltpu.VMEM((n_cols, rows, COLS), F32),
                pltpu.VMEM((n_cols, rows, COLS), F32),
                pltpu.VMEM((n_cols, rows, COLS), F32),
                dma((4,)), dma((9,)), dma((9,)),
                dma((n_own, 3)), dma((n_own, 3)),
                dma((n_z,)), dma((n_z,)), dma((n_z,)), dma((n_z,)),
                dma((n_z,)), dma((n_z,)), dma((n_z,)), dma((n_z,)),
                dma((3, n_cols, PIECES)), dma((3, n_cols, PIECES)),
            ],
            compiler_params=pltpu.CompilerParams(
                collective_id=0, has_side_effects=True, vmem_limit_bytes=67_043_328
            ),
        )(tokens, expert_ids.T, gates.T, w_gate, w_up, w_down)

    return jax.shard_map(local_layer, mesh=mesh, in_specs=(row_spec, row_spec, row_spec, P("ep", None, "tp"), P("ep", None, "tp"), P("ep", "tp", None)), out_specs=row_spec, check_vma=False)
```

```python
import functools

import jax
import jax.numpy as jnp
from jax import lax
from jax.experimental import pallas as pl
from jax.experimental.pallas import tpu as pltpu
from jax.sharding import PartitionSpec as P

MESH = pl.DeviceIdType.MESH
F32 = jnp.float32
BF16 = jnp.bfloat16

PIECES = 4
COLS = 256


def layer_kernel(
    tok_h, ids_ref, gates_ref, wg_h, wu_h, wd_h, out_ref,
    tok, raw, gm, wg, wu, wd, hid, acc, got_a, got_b, got_c,
    loc_sem, tok_ss, tok_rs, own_ss, own_rs, z_ss, z_rs, x_ss, x_rs, cz_ss, cz_rs, cx_ss, cx_rs, out_ss, out_rs,
):
    n_own, hidden, ff = wg_h.shape
    half = n_own // 2
    rows = tok_h.shape[0]
    part = rows // 2
    n_cols = hidden // COLS
    chunk = rows // PIECES
    top_k = ids_ref.shape[0]
    x = lax.axis_index("dp")
    z = lax.axis_index("tp")
    ep = lax.axis_index("ep")
    core = lax.rem(ep, 2)
    to_x = {"dp": 1 - x}
    to_y = {"ep": lax.rem(ep + 2, 4)}
    to_c = {"ep": ep + 1 - 2 * core}
    to_z = {"tp": z + 1 - 2 * lax.rem(z, 2)}
    to_zz = {"tp": lax.rem(z + 2, 4)}
    row_d, row_c, row_b, row_a = 0, rows, 2 * rows, 3 * rows

    def rcopy(src, dst, ss, rs, dev):
        return pltpu.make_async_remote_copy(
            src_ref=src, dst_ref=dst, send_sem=ss, recv_sem=rs, device_id=dev, device_id_type=MESH
        )

    bufs = (wg, wu, wd)
    hbm = (wg_h, wu_h, wd_h)

    loc = [pltpu.make_async_copy(tok_h, tok.at[pl.ds(row_d, rows)], loc_sem.at[0])]
    loc += [pltpu.make_async_copy(hbm[a], bufs[a].at[0, 0], loc_sem.at[1 + a]) for a in range(3)]
    for cp in loc:
        cp.start()
    raw[0, pl.ds(0, top_k)] = ids_ref[...].astype(F32)
    raw[0, pl.ds(top_k, top_k)] = gates_ref[...]

    barrier = pltpu.get_barrier_semaphore()
    for dev in (to_x, to_y, to_c, to_z, to_zz):
        pl.semaphore_signal(barrier, inc=1, device_id=dev, device_id_type=MESH)
    with jax.named_scope("entry"):
        pl.semaphore_wait(barrier, 5)

    def side(base, p):
        return pl.ds(base + p * part, part)

    tok_y = [rcopy(tok_h.at[side(0, p)], tok.at[side(row_c, p)], tok_ss.at[8 * p], tok_rs.at[8 * p], to_y)
             for p in range(2)]
    gat_y = rcopy(raw.at[0], raw.at[1], tok_ss.at[1], tok_rs.at[1], to_y)
    gat_z = rcopy(raw.at[0], raw.at[2], tok_ss.at[2], tok_rs.at[2], to_zz)
    gat_f = rcopy(raw.at[2], raw.at[3], tok_ss.at[3], tok_rs.at[3], to_y)
    tok_z = [rcopy(tok_h.at[side(0, p)], tok.at[side(row_b, p)], tok_ss.at[4 + p], tok_rs.at[4 + p], to_zz)
             for p in range(2)]
    tok_f = [rcopy(tok.at[side(row_b, p)], tok.at[side(row_a, p)], tok_ss.at[6 + p], tok_rs.at[6 + p], to_y)
             for p in range(2)]

    def own_c(i, a):
        return rcopy(hbm[a].at[i], bufs[a].at[0, 1, i], own_ss.at[i, a], own_rs.at[i, a], to_c)

    n_in = 2 * half
    n_z = n_in + n_cols

    def at_slot(share, n, lo):
        if n < n_in:
            return bufs[n % 2].at[1, share, lo + n // 2]
        return wd.at[1, share, pl.ds(lo, half), :, pl.ds((n - n_in) * COLS, COLS)]

    def over_z(n):
        if n < n_in:
            src = hbm[n % 2].at[x * half + n // 2]
        else:
            src = wd_h.at[pl.ds(x * half, half), :, pl.ds((n - n_in) * COLS, COLS)]
        return rcopy(src, at_slot(0, n, 0), z_ss.at[n], z_rs.at[n], to_z)

    def over_x(n):
        return rcopy(at_slot(0, n, 0), at_slot(0, n, half), x_ss.at[n], x_rs.at[n], to_x)

    def over_cz(n):
        return rcopy(at_slot(0, n, 0), at_slot(1, n, 0), cz_ss.at[n], cz_rs.at[n], to_c)

    def over_cx(n):
        return rcopy(at_slot(0, n, half), at_slot(1, n, half), cx_ss.at[n], cx_rs.at[n], to_c)

    inner_layer = lax.rem(z * (3 - z), 3) // 2
    tok_z[0].start()
    tok_y[0].start()
    gat_z.start()
    gat_y.start()
    tok_y[1].start()

    @pl.when(inner_layer == 0)
    def _():
        tok_z[1].start()

    for a in range(3):
        own_c(0, a).start()
    for n in range(n_z):
        over_z(n).start()
    for i in range(1, n_own):
        for a in range(3):
            own_c(i, a).start()

    base = (ep * n_own, (ep + 1 - 2 * core) * n_own)

    def gates_of(b):
        lane = lax.broadcasted_iota(jnp.int32, (2 * n_own, rows), 0)
        second_core = lane >= n_own
        t = jnp.where(second_core, lane - n_own, lane) + x * half
        t = jnp.where(t >= n_own, t - n_own, t)
        name = (t + jnp.where(second_core, base[1], base[0])).astype(F32)
        mine_of = jnp.zeros(name.shape, F32)
        for j in range(top_k):
            mine_of += jnp.where(name == raw[b, j : j + 1], raw[b, top_k + j : top_k + j + 1], 0.0)
        full = jnp.concatenate([mine_of, jnp.zeros((128 - 2 * n_own, rows), F32)], axis=0)
        gm[pl.ds(b * rows, rows)] = full.T

    with jax.named_scope("loc"):
        for cp in loc:
            cp.wait()
    gates_of(0)

    def slot(t):
        return (t % 2) * half + t // 2

    def inner(r, m, s, i):
        at = pl.ds(pl.multiple_of(r, m), m)
        xb = tok[at]
        for c in range(2):
            w_in = jnp.concatenate([wg[s, c, i], wu[s, c, i]], axis=1)
            both = jnp.dot(xb, w_in, preferred_element_type=F32)
            hid[s, c, i, at] = (jax.nn.silu(both[:, :ff]) * both[:, ff:]).astype(BF16)

    def first(r, m):
        def go(i, carry):
            inner(r, m, 0, i)
            return carry

        lax.fori_loop(0, n_own, go, 0)

    def second(r, m, lo, hi):
        def go(t, carry):
            inner(r, m, 1, slot(t))
            return carry

        lax.fori_loop(lo, hi, go, 0)

    def second_blocks(t, lo, hi):
        def go(b, carry):
            inner(b * rows, rows, 1, slot(t))
            return carry

        lax.fori_loop(lo, hi, go, 0)

    def down(r, k):
        at = pl.ds(r, rows)
        sl = pl.ds(pl.multiple_of(k * COLS, COLS), COLS)
        for q in range(n_own):
            i = lax.rem(x * half + q, n_own)
            total = None if q == 0 else acc[k, at]
            for c in range(2):
                h = jnp.concatenate([hid[0, c, i, at], hid[1, c, q, at]], axis=1)
                w_out = jnp.concatenate([wd[0, c, i, :, sl], wd[1, c, q, :, sl]], axis=0)
                lane = c * n_own + q
                term = gm[at, lane : lane + 1] * jnp.dot(h, w_out, preferred_element_type=F32)
                total = term if total is None else total + term
            acc[k, at] = total

    def pass_z(n):
        with jax.named_scope(f"ev_z{n}"):
            over_z(n).wait_recv()
        over_x(n).start()
        over_cz(n).start()

    def pass_x(n):
        with jax.named_scope(f"ev_x{n}"):
            over_x(n).wait_recv()
        over_cx(n).start()

    def ready(t):
        with jax.named_scope(f"ev_q{t}"):
            for n in (t - t % 2, t - t % 2 + 1):
                (over_cx(n) if t % 2 else over_cz(n)).wait_recv()

    def rows_of(j):
        return pl.ds(j * chunk, chunk)

    def out_copy(which, r, got, dev):
        def make(k, j):
            return rcopy(acc.at[k, pl.ds(r + j * chunk, chunk)], got.at[k, rows_of(j)],
                         out_ss.at[which, k, j], out_rs.at[which, k, j], dev)

        return make

    send_a = out_copy(0, row_a, got_a, to_y)
    send_b = out_copy(1, row_b, got_b, to_zz)
    send_c = out_copy(2, row_c, got_c, to_y)

    def add_a(k, j):
        with jax.named_scope(f"late_a{k}{j}"):
            send_a(k, j).wait_recv()
        at = pl.ds(row_b + j * chunk, chunk)
        acc[k, at] = acc[k, at] + got_a[k, rows_of(j)]
        send_b(k, j).start()

    def give(k, j):
        with jax.named_scope(f"late_c{k}{j}"):
            send_c(k, j).wait_recv()
        with jax.named_scope(f"late_b{k}{j}"):
            send_b(k, j).wait_recv()
        total = acc[k, rows_of(j)] + got_c[k, rows_of(j)] + got_b[k, rows_of(j)]
        out_ref[rows_of(j), pl.ds(k * COLS, COLS)] = total.astype(out_ref.dtype)

    def mine(i, carry):
        with jax.named_scope("ev_own"):
            for a in range(3):
                own_c(i, a).wait_recv()
        inner(row_d, rows, 0, i)
        return carry

    lax.fori_loop(0, n_own, mine, 0)

    def near_tokens(p):
        with jax.named_scope(f"ev_tok_c{p}"):
            tok_y[p].wait_recv()
            if p == 0:
                gat_y.wait_recv()
        if p == 0:
            gates_of(1)
        first(row_c + p * part, part)

    def b_tokens(p):
        with jax.named_scope(f"ev_tok_b{p}"):
            tok_z[p].wait_recv()
            if p == 0:
                gat_z.wait_recv()
        tok_f[p].start()
        if p == 0:
            gat_f.start()
            gates_of(2)

    def a_tokens(p):
        with jax.named_scope(f"ev_tok_a{p}"):
            tok_f[p].wait_recv()
            if p == 0:
                gat_f.wait_recv()
        if p == 0:
            gates_of(3)
        first(row_a + p * part, part)

    def middle():
        tok_z[1].start()
        near_tokens(0)
        near_tokens(1)
        b_tokens(0)
        pass_z(0)
        first(row_b, part)
        pass_z(1)
        ready(0)
        second_blocks(0, 0, 2)
        second(row_b, part, 0, 1)
        pass_z(2)
        a_tokens(0)
        pass_x(0)
        pass_x(1)
        b_tokens(1)
        pass_z(3)
        first(row_b + part, part)
        ready(1)
        second_blocks(1, 0, 2)
        second(row_b, part, 1, 2)
        second(row_b + part, part, 0, 2)
        pass_z(4)
        ready(2)
        second_blocks(2, 0, 3)
        pass_x(2)
        pass_x(3)
        second(row_a, part, 0, 3)
        pass_z(5)
        a_tokens(1)
        second(row_a + part, part, 0, 3)
        ready(3)
        second_blocks(3, 0, 2)
        pass_z(6)
        second_blocks(3, 2, 4)
        pass_x(4)
        pass_x(5)
        ready(4)
        second_blocks(4, 1, 4)
        pass_z(7)
        ready(5)
        second_blocks(5, 1, 4)
        ready(6)
        second_blocks(6, 2, 4)
        pass_z(8)
        pass_x(6)
        pass_x(7)
        ready(7)
        second_blocks(7, 2, 4)
        pass_z(9)

    def end():
        pass_z(0)
        near_tokens(0)
        pass_z(1)
        near_tokens(1)
        pass_z(2)
        pass_x(0)
        pass_x(1)
        ready(0)
        second_blocks(0, 0, 2)
        ready(1)
        second_blocks(1, 0, 2)
        b_tokens(0)
        first(row_b, part)
        second(row_b, part, 0, 2)
        b_tokens(1)
        pass_z(3)
        first(row_b + part, part)
        second(row_b + part, part, 0, 2)
        pass_z(4)
        a_tokens(0)
        second(row_a, part, 0, 2)
        ready(2)
        second_blocks(2, 1, 3)
        second(row_a, part, 2, 3)
        pass_x(2)
        pass_x(3)
        pass_z(5)
        ready(3)
        second_blocks(3, 1, 3)
        second(row_a, part, 3, 4)
        a_tokens(1)
        pass_z(6)
        second(row_a + part, part, 0, 4)
        pass_x(4)
        pass_x(5)
        ready(4)
        second_blocks(4, 1, 4)
        pass_z(7)
        ready(5)
        second_blocks(5, 1, 4)
        ready(6)
        second_blocks(6, 2, 4)
        pass_z(8)
        pass_x(6)
        pass_x(7)
        ready(7)
        second_blocks(7, 2, 4)
        pass_z(9)

    pl.when(inner_layer == 1)(middle)
    pl.when(inner_layer == 0)(end)

    def column(k, carry):
        for m in range(n_cols):
            @pl.when(k == m)
            def _(m=m):
                n = n_in + m
                if m == 0:
                    pass_x(n)
                with jax.named_scope(f"ev_w{m}"):
                    over_cz(n).wait_recv()
                    over_cx(n).wait_recv()

        down(row_a, k)
        with jax.named_scope("out_a"):
            for j in range(PIECES):
                send_a(k, j).start()

        @pl.when(k == 1)
        def _():
            add_a(0, 1)

        down(row_b, k)

        @pl.when(k == 0)
        def _():
            put_off = 2 + 2 * inner_layer
            second(row_d, rows, put_off, put_off + 3)
            add_a(0, 0)
            pass_z(n_in + 2)
            second(row_d, rows, put_off + 3, n_own)
            second(row_c, rows, n_own - 2, n_own)

        @pl.when(k == 1)
        def _():
            add_a(0, 2)

        @pl.when(k == 2)
        def _():
            add_a(0, 3)

        @pl.when(k == 3)
        def _():
            add_a(1, 0)
            add_a(1, 1)

        down(row_c, k)
        for now, blocks in ((1, (0,)), (2, (1,)), (3, (2, 3))):
            @pl.when(k == now)
            def _(blocks=blocks):
                for m in blocks:
                    for j in range(PIECES):
                        send_c(m, j).start()

        for m in range(1, n_cols):
            @pl.when(k == m - 1)
            def _(m=m):
                if m == 1:
                    pass_z(n_in + 3)
                pass_x(n_in + m)

        down(row_d, k)
        return carry

    lax.fori_loop(0, n_cols, column, 0)
    add_a(1, 2)
    add_a(1, 3)
    for add_k, give_k in ((2, 0), (3, 1), (None, 2), (None, 3)):
        for j in range(PIECES):
            if give_k is not None:
                give(give_k, j)
            if add_k is not None:
                add_a(add_k, j)

    for cp in [gat_y, gat_z, gat_f] + tok_y + tok_z + tok_f:
        cp.wait_send()
    for a in range(3):
        for i in range(n_own):
            own_c(i, a).wait_send()
    for n in range(n_z):
        for cp in (over_z(n), over_x(n), over_cz(n), over_cx(n)):
            cp.wait_send()
    for k in range(n_cols):
        for j in range(PIECES):
            for cp in (send_a(k, j), send_b(k, j), send_c(k, j)):
                cp.wait_send()


def solution(mesh):
    row_spec = P(("dp", "ep", "tp"), None)

    def local_layer(tokens, expert_ids, gates, w_gate, w_up, w_down):
        n_own = w_gate.shape[0]
        rows, hidden = tokens.shape
        ff = w_gate.shape[2]
        n_cols = hidden // COLS
        n_z = n_own + n_cols
        any_spec = pl.BlockSpec(memory_space=pl.ANY)
        vmem_spec = pl.BlockSpec(memory_space=pltpu.VMEM)
        dma = pltpu.SemaphoreType.DMA
        return pl.pallas_call(
            layer_kernel,
            out_shape=jax.ShapeDtypeStruct((rows, hidden), jnp.bfloat16),
            in_specs=[any_spec, vmem_spec, vmem_spec, any_spec, any_spec, any_spec],
            out_specs=vmem_spec,
            scratch_shapes=[
                pltpu.VMEM((4 * rows, hidden), BF16),
                pltpu.VMEM((4, 2 * expert_ids.shape[1], rows), F32),
                pltpu.VMEM((4 * rows, 128), F32),
                pltpu.VMEM((2, 2, n_own, hidden, ff), BF16),
                pltpu.VMEM((2, 2, n_own, hidden, ff), BF16),
                pltpu.VMEM((2, 2, n_own, ff, hidden), BF16),
                pltpu.VMEM((2, 2, n_own, 4 * rows, ff), BF16),
                pltpu.VMEM((n_cols, 4 * rows, COLS), F32),
                pltpu.VMEM((n_cols, rows, COLS), F32),
                pltpu.VMEM((n_cols, rows, COLS), F32),
                pltpu.VMEM((n_cols, rows, COLS), F32),
                dma((4,)), dma((9,)), dma((9,)),
                dma((n_own, 3)), dma((n_own, 3)),
                dma((n_z,)), dma((n_z,)), dma((n_z,)), dma((n_z,)),
                dma((n_z,)), dma((n_z,)), dma((n_z,)), dma((n_z,)),
                dma((3, n_cols, PIECES)), dma((3, n_cols, PIECES)),
            ],
            compiler_params=pltpu.CompilerParams(
                collective_id=0, has_side_effects=True, vmem_limit_bytes=67_043_328
            ),
        )(tokens, expert_ids.T, gates.T, w_gate, w_up, w_down)

    return jax.shard_map(local_layer, mesh=mesh, in_specs=(row_spec, row_spec, row_spec, P("ep", None, "tp"), P("ep", None, "tp"), P("ep", "tp", None)), out_specs=row_spec, check_vma=False)
```
